128 devices in a mesh: shard: 128 (over y, z, x, core).
Axes of the slice: x: 4, y: 4, z: 4, core: 2. Of those that a mesh axis runs over, the one named last changes fastest.
Arguments:
- lookup_ids: int32 [32768, 4, 8], P('shard'), may hold values from 0 to 524287, as said below
- bag_lengths: int32 [32768, 4], P('shard'), may hold values from 1 to 8
- pooled_gradients: bfloat16 [32768, 4, 128], P('shard'), may hold values from -6 to 6
- tables: float32 [4, 524288, 128], P(None, 'shard'), may hold values from -4 to 4
- accumulators: float32 [4, 524288], P(None, 'shard'), may hold values from 0.05 to 2
Outputs:
- new_tables: float32 [4, 524288, 128], P(None, 'shard')
- new_accumulators: float32 [4, 524288], P(None, 'shard')
- gradient_scale: float32 [], replicated
The draws below stay inside these ranges and needn't reach their ends.
Inputs may be any that keep to these rules, and one draw needn't show every extreme that they name: `lookup_ids`: row ids are rows 0 to 524287 of their table. Among the 256 x 8 entries of one table held by one device (padding positions included), the rows of every owning device's block of 4096 rows are named exactly 16 times. About half the lookups fall on the first 32 rows of an owner's block.
All inputs are finite; a program needn't handle non-finite values.
Results may differ from the reference program's by a relative error of at most 0.0003.
Values may be sent and summed in bfloat16 or wider, within the bound.
A program may use at most 128 MiB of HBM per device.

```python
import math
import jax
import jax.numpy as jnp
from jax import lax

E = 128
NT = 4
L = 8
HOT = 32
B_DEV = 256
ROWS_DEV = 4096
BATCH = 32768
ROWS = 524288


def draw_lookup_ids(key, part):
    peer_count = BATCH // B_DEV
    lookups = B_DEV * L

    def one_block(block_key):
        first_key, second_key, third_key, fourth_key = jax.random.split(block_key, 4)
        shuffled = jax.random.permutation(first_key, lookups)
        owners = shuffled % peer_count
        cold_rows = jax.random.randint(second_key, (lookups,), 0, ROWS_DEV)
        hot_rows = jax.random.randint(third_key, (lookups,), 0, min(HOT, ROWS_DEV))
        chooser = jax.random.randint(fourth_key, (lookups,), 0, 2)
        local_rows = jnp.where(chooser == 1, hot_rows, cold_rows)
        return (owners * ROWS_DEV + local_rows).astype(jnp.int32)
    block_keys = jax.random.split(jax.random.fold_in(key, 17), peer_count * NT)
    blocks = jax.vmap(one_block)(block_keys)
    blocks = blocks.reshape(peer_count, NT, B_DEV, L).transpose(0, 2, 1, 3)
    return blocks.reshape(BATCH, NT, L)


def touch_ends(array, key, low, high):
    dims = array.shape
    spot = [jax.random.randint(jax.random.fold_in(key, axis), (), 0, dims[axis]) for axis in range(len(dims))]
    array = array.at[tuple(spot)].set(low)
    longest = dims.index(max(dims))
    spot[longest] = (spot[longest] + 1) % dims[longest]
    return array.at[tuple(spot)].set(high)


def block_scale(stream_key, dims, shards, low, largest):
    def one(dim, blocks):
        steps = jax.random.uniform(jax.random.fold_in(jax.random.fold_in(stream_key, 6), dim), (blocks,), jnp.float32, low / len(shards), largest / len(shards))
        return jnp.repeat(jnp.exp(steps), dims[dim] // blocks).reshape((-1,) + (1,) * (len(dims) - dim - 1))

    level = one(*shards[0])
    for cut in shards[1:]:
        level = level * one(*cut)
    return level


def bell_draw(stream_key, dims, width, most, shards=(), kind=jnp.bfloat16):
    loudness = block_scale(stream_key, dims, shards, -0.22, 0.18) if shards else 1.0
    array = jax.random.normal(stream_key, dims, jnp.float32) * width * loudness
    return jnp.minimum(jnp.maximum(array, -most), most).astype(kind)


def setup_inputs(seed: int = 0) -> dict:
    key_list = jax.random.split(jax.random.key(seed), 6)
    lookup_ids = draw_lookup_ids(jax.random.fold_in(key_list[5], 71), 0)
    bag_lengths = touch_ends(jax.random.randint(key_list[1], (BATCH, NT), 1, L + 1), jax.random.fold_in(key_list[1], 1), 1, L).astype(jnp.int32)
    pooled_gradients = bell_draw(key_list[2], (BATCH, NT, E), 1.0, 6.0, ((0, 128),))
    tables = bell_draw(key_list[3], (NT, ROWS, E), 0.5, 4.0, ((1, 128),), jnp.float32)
    accumulators = jnp.clip(jnp.exp(math.log(2.0) - 3.6888794 * jax.random.uniform(key_list[4], (NT, ROWS), jnp.float32) ** block_scale(key_list[4], (NT, ROWS), ((1, 128),), -0.2, 0.2)), 0.05, 2.0)
    return {"lookup_ids": lookup_ids, "bag_lengths": bag_lengths, "pooled_gradients": pooled_gradients, "tables": tables, "accumulators": accumulators}


step_size = 0.5
epsilon = 1e-08

def reference(lookup_ids, bag_lengths, pooled_gradients, tables, accumulators):
    position = jnp.arange(L, dtype=jnp.int32)
    inside = position[None, None, :] < bag_lengths[:, :, None]
    scaled = (pooled_gradients.astype(jnp.float32) / bag_lengths[:, :, None].astype(jnp.float32)).astype(jnp.bfloat16)
    scaled = lax.optimization_barrier(scaled).astype(jnp.float32)

    def per_table(pieces):
        rows_here, inside_here, scaled_here, table_here, accum_here = pieces
        terms = jnp.where(inside_here[:, :, None], scaled_here[:, None, :], jnp.float32(0.0)).reshape(-1, E)
        summed = jax.ops.segment_sum(terms, rows_here.reshape(-1).astype(jnp.int32), num_segments=ROWS)
        mean_square = lax.optimization_barrier(jnp.mean(summed * summed, axis=1))
        new_accum = accum_here + mean_square
        new_table = table_here - step_size * summed / (jnp.sqrt(new_accum)[:, None] + epsilon)
        return (new_table, new_accum, jnp.sum(summed * summed))
    pieces = (lookup_ids.transpose(1, 0, 2), inside.transpose(1, 0, 2), scaled.transpose(1, 0, 2), tables, accumulators)
    new_tables, new_accumulators, squares = lax.map(per_table, pieces)
    gradient_scale = jnp.sqrt(jnp.sum(squares) / (E * NT * BATCH * L))
    return (new_tables, new_accumulators, gradient_scale)
```

```python
import functools

import jax
import jax.numpy as jnp
from jax import lax
from jax.experimental import pallas as pl
from jax.experimental.pallas import tpu as pltpu
from jax.sharding import PartitionSpec as P

STEP = 0.5
EPS = 1e-08
F32 = jnp.float32
BF16 = jnp.bfloat16
I32 = jnp.int32
MESH = pl.DeviceIdType.MESH
VMEM = pltpu.VMEM


def iota(shape, dim):
    return lax.broadcasted_iota(I32, shape, dim)


def one_if(mask):
    return jnp.where(mask, F32(1.0), F32(0.0)).astype(BF16)


def nt_dot(a, b):
    return lax.dot_general(a, b, (((1,), (1,)), ((), ())), preferred_element_type=F32)


def signal_all(peers):
    me = lax.axis_index("shard")
    barrier = pltpu.get_barrier_semaphore()

    def one(k, carry):
        pl.semaphore_signal(
            barrier, inc=1, device_id=(lax.rem(me + k, peers),), device_id_type=MESH
        )
        return carry

    lax.fori_loop(1, peers, one, 0)
    return barrier


def pack_table(t, ids_ref, len_ref, g32_ref, send_ref, rows32_ref, shift, bucket):
    bags = ids_ref.shape[2]
    width = ids_ref.shape[1]
    peers = send_ref.shape[0]
    lens = len_ref[t : t + 1, :]
    owner_iota = iota((peers, bags), 0)
    bag_iota = iota((1, bags), 1).astype(F32)
    upper = one_if(iota((bags, bags), 0) < iota((bags, bags), 1))
    ones = jnp.ones((bags, bags), BF16)
    prefix_rhs = jnp.concatenate([upper, ones], axis=0)
    rank_iota = iota((bucket, bags), 0).astype(F32)
    seen = jnp.zeros((peers, bags), F32)
    owned = []
    values = []
    for l in range(width):
        ids = ids_ref[t, l : l + 1, :]
        owner = lax.shift_right_logical(ids, shift)
        local = lax.bitwise_and(ids, (1 << shift) - 1)
        own32 = jnp.where(owner == owner_iota, F32(1.0), F32(0.0))
        own = own32.astype(BF16)
        before = jnp.dot(
            jnp.concatenate([own, seen.astype(BF16)], axis=1),
            prefix_rhs,
            preferred_element_type=F32,
        )
        rank = jnp.sum(own32 * before, axis=0, keepdims=True)
        seen = seen + own32
        at_rank = rank == rank_iota
        bag = jnp.where(l < lens, bag_iota, F32(bags))
        high = lax.shift_right_logical(local, 6).astype(F32)
        low = lax.bitwise_and(local, 63).astype(F32)
        zero = jnp.zeros_like(rank_iota)
        values.append(
            jnp.concatenate(
                [
                    jnp.where(at_rank, bag, zero),
                    jnp.where(at_rank, high, zero),
                    jnp.where(at_rank, low, zero),
                ],
                axis=0,
            ).astype(BF16)
        )
        owned.append(own)
    table = nt_dot(jnp.concatenate(owned, axis=1), jnp.concatenate(values, axis=1))
    bag_of = table[:, :bucket]
    rows = (table[:, bucket : 2 * bucket] * 64.0 + table[:, 2 * bucket :]).astype(I32)
    lane = iota((peers, bags), 1).astype(F32)
    select = jnp.concatenate([one_if(bag_of[:, r : r + 1] == lane) for r in range(bucket)], axis=0)
    scaled = g32_ref[t]
    moved = jnp.dot(select, scaled, preferred_element_type=F32)
    for r in range(bucket):
        rows32_ref[pl.ds(r, peers, stride=bucket), :] = moved[r * peers : (r + 1) * peers]
    send_ref[:, t * bucket : (t + 1) * bucket, :] = (
        rows32_ref[...].reshape(peers, bucket, -1).astype(BF16)
    )
    return rows


def exchange_kernel(
    shift,
    bucket,
    ids_ref,
    len_ref,
    g_ref,
    got_ref,
    grow_ref,
    send_ref,
    srow_ref,
    g32_ref,
    scaled_ref,
    rows32_ref,
    send_sem,
    recv_sem,
):
    tables = ids_ref.shape[0]
    bags = ids_ref.shape[2]
    peers = send_ref.shape[0]
    me = lax.axis_index("shard")
    barrier = signal_all(peers)

    g32_ref[...] = g_ref[...].astype(F32)
    lens = len_ref[...].astype(F32)
    lens_t = jnp.concatenate([lens, jnp.ones((128 - tables, bags), F32)], axis=0).T
    for t in range(tables):
        part = g32_ref[pl.ds(t, bags, stride=tables), :]
        scaled_ref[t] = (part / lens_t[:, t : t + 1]).astype(BF16)
    rows = [
        pack_table(t, ids_ref, len_ref, scaled_ref, send_ref, rows32_ref, shift, bucket)
        for t in range(tables)
    ]
    rows.append(jnp.zeros((peers, 128 - tables * bucket), I32))
    srow_ref[...] = jnp.concatenate(rows, axis=1).reshape(srow_ref.shape)

    got_ref[pl.ds(me, 1)] = send_ref[pl.ds(me, 1)]
    grow_ref[pl.ds(me, 1)] = srow_ref[pl.ds(me, 1)]
    pl.semaphore_wait(barrier, peers - 1)

    def send(k, carry):
        p = lax.rem(me + k, peers)
        for i, (src, dst) in enumerate(((srow_ref, grow_ref), (send_ref, got_ref))):
            pltpu.make_async_remote_copy(
                src_ref=src.at[p],
                dst_ref=dst.at[me],
                send_sem=send_sem.at[i],
                recv_sem=recv_sem.at[i],
                device_id=(p,),
                device_id_type=MESH,
            ).start()
        return carry

    lax.fori_loop(1, peers, send, 0)
    others = pl.ds(0, peers - 1)
    for i, (src, dst) in enumerate(((srow_ref, grow_ref), (send_ref, got_ref))):
        pltpu.make_async_copy(dst.at[others], dst.at[others], recv_sem.at[i]).wait()
        pltpu.make_async_copy(src.at[others], src.at[others], send_sem.at[i]).wait()


def update_kernel(
    bucket,
    got_ref,
    grow_ref,
    acc_ref,
    tab_ref,
    out_ref,
    nacc_ref,
    part_ref,
    tab_vm,
    out_vm,
    low_vm,
    hot_vm,
    rhs_vm,
    square_ref,
    in_sem,
    out_sem,
):
    tables, rows, width = tab_ref.shape
    peers = got_ref.shape[0]
    lookups = peers * bucket
    group = 256 // bucket
    chunks = peers // group
    half = rows // 2
    tiles = half // 256
    loads = [
        pltpu.make_async_copy(tab_ref.at[t], tab_vm.at[t], in_sem.at[t]) for t in range(tables)
    ]
    for load in loads:
        load.start()

    got_rows = grow_ref[...].reshape(peers, 128)
    used = tables * bucket
    upper = lax.shift_right_logical(got_rows, half.bit_length() - 1)
    tile = lax.shift_right_logical(lax.bitwise_and(got_rows, half - 1), 8)
    low = lax.bitwise_and(got_rows, 255)
    spread_lane = iota((128, 256 * tables), 1)
    spread = one_if(
        iota((128, 256 * tables), 0)
        == lax.shift_right_logical(spread_lane, 8) * bucket
        + lax.bitwise_and(spread_lane, bucket - 1)
    )
    lane = iota((peers, 256 * tables), 1)
    own_lane = lax.shift_right_logical(
        lax.bitwise_and(lane, 255), bucket.bit_length() - 1
    ) == lax.bitwise_and(iota((peers, 256 * tables), 0), group - 1)

    def lane_vectors(digit):
        wide = jnp.dot(digit.astype(BF16), spread, preferred_element_type=F32)
        wide = jnp.where(own_lane, wide, F32(0.0)).reshape(chunks, group, 256 * tables)
        return jnp.sum(wide, axis=1)

    lows = lane_vectors(low)
    tiles_of = lane_vectors(tile)
    uppers = lane_vectors(upper)
    upper_t = jnp.concatenate(
        [uppers[:, i * 128 : (i + 1) * 128] for i in range(2 * tables)]
        + [jnp.zeros((128 - 2 * tables * chunks, 128), F32)],
        axis=0,
    ).T
    square_ref[...] = jnp.zeros_like(square_ref)
    acc_t = acc_ref[...].T
    lane_id = iota((128, 128), 1)
    sub_id = iota((256, 256), 0).astype(F32)

    stores = []
    for t in range(tables):
        for c in range(chunks):
            col = slice(c * 256, (c + 1) * 256)
            low_vm[:, col] = one_if(lows[c : c + 1, t * 256 : (t + 1) * 256] == sub_id)
            hot_vm[:, col] = jnp.broadcast_to(
                tiles_of[c : c + 1, t * 256 : (t + 1) * 256], (16, 256)
            ).astype(BF16)
            for h in range(2):
                k = 2 * t + h
                is_upper = upper_t[:, k * chunks + c : k * chunks + c + 1]
                src = slice(c * group + h * group // 2, c * group + (h + 1) * group // 2)
                terms = got_ref[src, t * bucket : (t + 1) * bucket, :].reshape(128, width)
                up = jnp.broadcast_to(is_upper, (128, width)).astype(BF16)
                row = slice(c * 256 + h * 128, c * 256 + (h + 1) * 128)
                rhs_vm[row, width:] = terms * up
                rhs_vm[row, :width] = terms * (BF16(1.0) - up)
        loads[t].wait()

        def tile_step(m, carry, t=t):
            mask = jnp.where(
                hot_vm[...] == m.astype(F32).astype(BF16), BF16(1.0), BF16(0.0)
            )
            lhs = (low_vm[...].reshape(16, 16, lookups) * mask[None]).reshape(256, lookups)
            both = jnp.dot(lhs, rhs_vm[...], preferred_element_type=F32)
            for p in range(2):
                for h in range(2):
                    s = both[h * 128 : (h + 1) * 128, p * width : (p + 1) * width]
                    block = p * (half // 128) + 2 * m + h
                    out_vm[t, pl.ds(pl.multiple_of(block * 128, 128), 128), :] = s
                    squares = jnp.sum(s * s, axis=1, keepdims=True)
                    square_ref[...] = jnp.where(
                        lane_id == block * tables + t, squares, square_ref[...]
                    )
            return carry

        lax.fori_loop(0, tiles, tile_step, 0)
        new_acc = acc_t + square_ref[...] * F32(1.0 / width)
        rate = STEP / (jnp.sqrt(new_acc) + EPS)
        for block in range(rows // 128):
            at = slice(block * 128, (block + 1) * 128)
            lane_at = block * tables + t
            out_vm[t, at, :] = tab_vm[t, at, :] - out_vm[t, at, :] * rate[:, lane_at : lane_at + 1]
        store = pltpu.make_async_copy(out_vm.at[t], out_ref.at[t], out_sem.at[t])
        store.start()
        stores.append(store)
    nacc_ref[...] = (acc_t + square_ref[...] * F32(1.0 / width)).T
    part_ref[...] = jnp.broadcast_to(
        jnp.sum(jnp.sum(square_ref[...], axis=1, keepdims=True), axis=0, keepdims=True), (8, 128)
    )
    for store in stores:
        store.wait()


def total_kernel(count, part_ref, out_ref, got_ref, send_sem, recv_sem):
    peers = got_ref.shape[0]
    me = lax.axis_index("shard")
    barrier = signal_all(peers)
    got_ref[pl.ds(me, 1)] = part_ref[0:1].reshape(1, 1, 128)
    pl.semaphore_wait(barrier, peers - 1)

    def send(k, carry):
        p = lax.rem(me + k, peers)
        pltpu.make_async_remote_copy(
            src_ref=part_ref.at[pl.ds(0, 1)],
            dst_ref=got_ref.at[me],
            send_sem=send_sem,
            recv_sem=recv_sem,
            device_id=(p,),
            device_id_type=MESH,
        ).start()
        return carry

    lax.fori_loop(1, peers, send, 0)
    others = pl.ds(0, peers - 1)
    pltpu.make_async_copy(got_ref.at[others], got_ref.at[others], recv_sem).wait()
    pltpu.make_async_copy(got_ref.at[others], got_ref.at[others], send_sem).wait()
    total = jnp.sum(got_ref[...].reshape(peers, 128), axis=0, keepdims=True)
    out_ref[...] = jnp.broadcast_to(jnp.sqrt(total * F32(1.0 / count)), out_ref.shape)


def per_device(peers, lookup_ids, bag_lengths, pooled_gradients, tables, accumulators):
    samples, count_tables, bag_width = lookup_ids.shape
    width = pooled_gradients.shape[2]
    rows_dev = tables.shape[1]
    lookups = samples * bag_width
    bucket = lookups // peers
    blocks = rows_dev // 128
    in_vmem = pl.BlockSpec(memory_space=VMEM)
    in_any = pl.BlockSpec(memory_space=pl.ANY)
    got, got_rows = pl.pallas_call(
        functools.partial(exchange_kernel, rows_dev.bit_length() - 1, bucket),
        out_shape=(
            jax.ShapeDtypeStruct((peers, count_tables * bucket, width), BF16),
            jax.ShapeDtypeStruct((peers, 1, 128), I32),
        ),
        in_specs=[in_vmem] * 3,
        out_specs=(in_vmem, in_vmem),
        scratch_shapes=[
            VMEM((peers, count_tables * bucket, width), BF16),
            VMEM((peers, 1, 128), I32),
            VMEM((samples * count_tables, width), F32),
            VMEM((count_tables, samples, width), BF16),
            VMEM((peers * bucket, width), F32),
            pltpu.SemaphoreType.DMA((2,)),
            pltpu.SemaphoreType.DMA((2,)),
        ],
        compiler_params=pltpu.CompilerParams(collective_id=0, has_side_effects=True),
        name="exchange",
    )(
        lookup_ids.transpose(1, 2, 0),
        bag_lengths.T,
        pooled_gradients.reshape(samples * count_tables, width),
    )
    acc = accumulators.reshape(count_tables, blocks, 128).transpose(1, 0, 2).reshape(-1, 128)
    new_tables, new_acc, part = pl.pallas_call(
        functools.partial(update_kernel, bucket),
        out_shape=(
            jax.ShapeDtypeStruct(tables.shape, F32),
            jax.ShapeDtypeStruct(acc.shape, F32),
            jax.ShapeDtypeStruct((8, 128), F32),
        ),
        in_specs=[in_vmem] * 3 + [in_any],
        out_specs=(in_any, in_vmem, in_vmem),
        scratch_shapes=[
            VMEM(tables.shape, F32),
            VMEM(tables.shape, F32),
            VMEM((256, lookups), BF16),
            VMEM((16, lookups), BF16),
            VMEM((lookups, 2 * width), BF16),
            VMEM((128, 128), F32),
            pltpu.SemaphoreType.DMA((count_tables,)),
            pltpu.SemaphoreType.DMA((count_tables,)),
        ],
        name="update",
    )(got, got_rows, acc, tables)
    new_acc = new_acc.reshape(blocks, count_tables, 128).transpose(1, 0, 2).reshape(accumulators.shape)
    count = width * count_tables * lookups * peers
    total = pl.pallas_call(
        functools.partial(total_kernel, count),
        out_shape=jax.ShapeDtypeStruct((8, 128), F32),
        in_specs=[in_vmem],
        out_specs=in_vmem,
        scratch_shapes=[
            VMEM((peers, 1, 128), F32),
            pltpu.SemaphoreType.DMA,
            pltpu.SemaphoreType.DMA,
        ],
        compiler_params=pltpu.CompilerParams(collective_id=1, has_side_effects=True),
        name="total",
    )(part)
    return (new_tables, new_acc, total[0, 0])


def solution(mesh):
    peers = mesh.devices.size
    return jax.shard_map(
        functools.partial(per_device, peers),
        mesh=mesh,
        in_specs=(
            P("shard", None, None),
            P("shard", None),
            P("shard", None, None),
            P(None, "shard", None),
            P(None, "shard"),
        ),
        out_specs=(P(None, "shard", None), P(None, "shard"), P()),
        check_vma=False,
    )
```

```python
import functools

import jax
import jax.numpy as jnp
from jax import lax
from jax.experimental import pallas as pl
from jax.experimental.pallas import tpu as pltpu
from jax.sharding import PartitionSpec as P

STEP = 0.5
EPS = 1e-08
F32 = jnp.float32
BF16 = jnp.bfloat16
I32 = jnp.int32
MESH = pl.DeviceIdType.MESH
VMEM = pltpu.VMEM


def iota(shape, dim):
    return lax.broadcasted_iota(I32, shape, dim)


def one_if(mask):
    return jnp.where(mask, F32(1.0), F32(0.0)).astype(BF16)


def nt_dot(a, b):
    return lax.dot_general(a, b, (((1,), (1,)), ((), ())), preferred_element_type=F32)


def signal_all(peers):
    me = lax.axis_index("shard")
    barrier = pltpu.get_barrier_semaphore()

    def one(k, carry):
        pl.semaphore_signal(
            barrier, inc=1, device_id=(lax.rem(me + k, peers),), device_id_type=MESH
        )
        return carry

    lax.fori_loop(1, peers, one, 0)
    return barrier


def rank_table(t, ids_ref, len_ref, peers, shift, bucket):
    bags = ids_ref.shape[2]
    width = ids_ref.shape[1]
    lens = len_ref[t : t + 1, :]
    owner_iota = iota((peers, bags), 0)
    bag_iota = iota((1, bags), 1).astype(F32)
    upper = one_if(iota((bags, bags), 0) < iota((bags, bags), 1))
    ones = jnp.ones((bags, bags), BF16)
    prefix_rhs = jnp.concatenate([upper, ones], axis=0)
    rank_iota = iota((bucket, bags), 0).astype(F32)
    seen = jnp.zeros((peers, bags), F32)
    owned = []
    values = []
    for l in range(width):
        ids = ids_ref[t, l : l + 1, :]
        owner = lax.shift_right_logical(ids, shift)
        local = lax.bitwise_and(ids, (1 << shift) - 1)
        own32 = jnp.where(owner == owner_iota, F32(1.0), F32(0.0))
        own = own32.astype(BF16)
        before = jnp.dot(
            jnp.concatenate([own, seen.astype(BF16)], axis=1),
            prefix_rhs,
            preferred_element_type=F32,
        )
        rank = jnp.sum(own32 * before, axis=0, keepdims=True)
        seen = seen + own32
        at_rank = rank == rank_iota
        bag = jnp.where(l < lens, bag_iota, F32(bags))
        high = lax.shift_right_logical(local, 6).astype(F32)
        low = lax.bitwise_and(local, 63).astype(F32)
        zero = jnp.zeros_like(rank_iota)
        values.append(
            jnp.concatenate(
                [
                    jnp.where(at_rank, bag, zero),
                    jnp.where(at_rank, high, zero),
                    jnp.where(at_rank, low, zero),
                ],
                axis=0,
            ).astype(BF16)
        )
        owned.append(own)
    table = nt_dot(jnp.concatenate(owned, axis=1), jnp.concatenate(values, axis=1))
    rows = (table[:, bucket : 2 * bucket] * 64.0 + table[:, 2 * bucket :]).astype(I32)
    return table[:, :bucket], rows


def select_table(t, bag_of, scaled_ref, send_ref, rows32_ref):
    peers, bucket = bag_of.shape
    bags = scaled_ref.shape[1]
    lane = iota((peers, bags), 1).astype(F32)
    select = jnp.concatenate([one_if(bag_of[:, r : r + 1] == lane) for r in range(bucket)], axis=0)
    moved = jnp.dot(select, scaled_ref[t], preferred_element_type=F32)
    for r in range(bucket):
        rows32_ref[pl.ds(r, peers, stride=bucket), :] = moved[r * peers : (r + 1) * peers]
    send_ref[t] = rows32_ref[...].reshape(peers, bucket, -1).astype(BF16)


def exchange_and_update(
    sizes,
    stride,
    shift,
    bucket,
    count,
    ids_hbm,
    len_hbm,
    g_hbm,
    acc_hbm,
    tab_ref,
    out_ref,
    nacc_ref,
    scale_ref,
    ids_ref,
    len_ref,
    g_ref,
    acc_ref,
    send_ref,
    srow_ref,
    got_ref,
    grow_ref,
    g32_ref,
    scaled_ref,
    rows32_ref,
    sum_ref,
    low_ref,
    hot_ref,
    rhs_ref,
    square_ref,
    part_ref,
    parts_ref,
    in_sem,
    send_sem,
    recv_sem,
):
    tables, rows, width = tab_ref.shape
    bags = ids_ref.shape[2]
    peers = send_ref.shape[1]
    lookups = peers * bucket
    group = 256 // bucket
    chunks = peers // group
    half = rows // 2
    tiles = half // 256
    me = lax.axis_index("shard")
    loads = [
        pltpu.make_async_copy(tab_ref.at[t], out_ref.at[t], in_sem.at[t]) for t in range(tables)
    ]
    small = [
        pltpu.make_async_copy(src, dst, in_sem.at[tables + i])
        for i, (src, dst) in enumerate(
            ((ids_hbm, ids_ref), (len_hbm, len_ref), (g_hbm, g_ref), (acc_hbm, acc_ref))
        )
    ]
    for load in small + loads:
        load.start()
    barrier = signal_all(peers)
    for load in small:
        load.wait()

    g32_ref[...] = g_ref[...].astype(F32)
    lens = len_ref[...].astype(F32)
    lens_t = jnp.concatenate([lens, jnp.ones((128 - tables, bags), F32)], axis=0).T
    for t in range(tables):
        part = g32_ref[pl.ds(t, bags, stride=tables), :]
        scaled_ref[t] = (part / lens_t[:, t : t + 1]).astype(BF16)
    ranked = [rank_table(t, ids_ref, len_ref, peers, shift, bucket) for t in range(tables)]
    srow_ref[...] = jnp.concatenate(
        [r for _, r in ranked] + [jnp.zeros((peers, 128 - tables * bucket), I32)], axis=1
    ).reshape(srow_ref.shape)

    near = []
    span = peers
    for size in sizes:
        span //= size
        here = lax.rem(lax.div(me, span), size)
        near.append([lax.rem(here + d, size) * span for d in range(size)])

    def peer_at(slot):
        offset = (stride * slot) % (peers - 1) + 1
        span = peers
        where = None
        for size, spots in zip(sizes, near):
            span //= size
            spot = spots[offset // span % size]
            where = spot if where is None else where + spot
        return where

    def send_all(src, dst, s):
        for slot in range(peers - 1):
            p = peer_at(slot)
            pltpu.make_async_remote_copy(
                src_ref=src(p),
                dst_ref=dst(slot),
                send_sem=send_sem.at[s],
                recv_sem=recv_sem.at[s],
                device_id=(p,),
                device_id_type=MESH,
            ).start()

    def send_table(t):
        send_all(lambda p: send_ref.at[t, p], lambda slot: got_ref.at[t, slot], t)

    others = pl.ds(0, peers - 1)

    select_table(0, ranked[0][0], scaled_ref, send_ref, rows32_ref)
    select_table(1, ranked[1][0], scaled_ref, send_ref, rows32_ref)
    pl.semaphore_wait(barrier, peers - 1)
    send_all(lambda p: srow_ref.at[p], lambda slot: grow_ref.at[slot], tables)
    send_table(0)
    for t in range(2, tables):
        select_table(t, ranked[t][0], scaled_ref, send_ref, rows32_ref)
        send_table(t - 1)
    grow_ref[pl.ds(peers - 1, 1)] = srow_ref[pl.ds(me, 1)]
    for t in range(tables):
        got_ref[t, pl.ds(peers - 1, 1)] = send_ref[t, pl.ds(me, 1)]
    send_table(tables - 1)
    acc_t = acc_ref[...].T
    square_ref[...] = jnp.zeros_like(square_ref)

    pltpu.make_async_copy(
        grow_ref.at[others], grow_ref.at[others], recv_sem.at[tables]
    ).wait()
    got_rows = grow_ref[...].reshape(peers, 128)
    upper = lax.shift_right_logical(got_rows, half.bit_length() - 1)
    tile = lax.shift_right_logical(lax.bitwise_and(got_rows, half - 1), 8)
    low = lax.bitwise_and(got_rows, 255)
    spread_lane = iota((128, 256 * tables), 1)
    spread = one_if(
        iota((128, 256 * tables), 0)
        == lax.shift_right_logical(spread_lane, 8) * bucket
        + lax.bitwise_and(spread_lane, bucket - 1)
    )
    lane = iota((peers, 256 * tables), 1)
    own_lane = lax.shift_right_logical(
        lax.bitwise_and(lane, 255), bucket.bit_length() - 1
    ) == lax.bitwise_and(iota((peers, 256 * tables), 0), group - 1)

    def lane_vectors(digit):
        wide = jnp.dot(digit.astype(BF16), spread, preferred_element_type=F32)
        wide = jnp.where(own_lane, wide, F32(0.0)).reshape(chunks, group, 256 * tables)
        return jnp.sum(wide, axis=1)

    lows = lane_vectors(low)
    tiles_of = lane_vectors(tile)
    uppers = lane_vectors(upper)
    upper_t = jnp.concatenate(
        [uppers[:, i * 128 : (i + 1) * 128] for i in range(2 * tables)]
        + [jnp.zeros((128 - 2 * tables * chunks, 128), F32)],
        axis=0,
    ).T
    lane_id = iota((128, 128), 1)
    sub_id = iota((256, 256), 0).astype(F32)

    for t in range(tables):
        for c in range(chunks):
            col = slice(c * 256, (c + 1) * 256)
            low_ref[:, col] = one_if(lows[c : c + 1, t * 256 : (t + 1) * 256] == sub_id)
            hot_ref[:, col] = jnp.broadcast_to(
                tiles_of[c : c + 1, t * 256 : (t + 1) * 256], (16, 256)
            ).astype(BF16)
        pltpu.make_async_copy(
            got_ref.at[t, others], got_ref.at[t, others], recv_sem.at[t]
        ).wait()
        for c in range(chunks):
            for h in range(2):
                k = 2 * t + h
                is_upper = upper_t[:, k * chunks + c : k * chunks + c + 1]
                src = slice(c * group + h * group // 2, c * group + (h + 1) * group // 2)
                terms = got_ref[t, src].reshape(128, width)
                up = jnp.broadcast_to(is_upper, (128, width)).astype(BF16)
                row = slice(c * 256 + h * 128, c * 256 + (h + 1) * 128)
                rhs_ref[row, width:] = terms * up
                rhs_ref[row, :width] = terms * (BF16(1.0) - up)

        def tile_step(m, carry, t=t):
            mask = jnp.where(hot_ref[...] == m.astype(F32).astype(BF16), BF16(1.0), BF16(0.0))
            lhs = (low_ref[...].reshape(16, 16, lookups) * mask[None]).reshape(256, lookups)
            both = jnp.dot(lhs, rhs_ref[...], preferred_element_type=F32)
            for p in range(2):
                for h in range(2):
                    s = both[h * 128 : (h + 1) * 128, p * width : (p + 1) * width]
                    block = p * (half // 128) + 2 * m + h
                    sum_ref[pl.ds(pl.multiple_of(block * 128, 128), 128), :] = s
                    squares = jnp.sum(s * s, axis=1, keepdims=True)
                    square_ref[...] = jnp.where(
                        lane_id == block * tables + t, squares, square_ref[...]
                    )
            return carry

        lax.fori_loop(0, tiles, tile_step, 0)
        if t == tables - 1:
            part_ref[...] = jnp.broadcast_to(
                jnp.sum(square_ref[...], axis=0, keepdims=True), part_ref.shape
            )
        new_acc = acc_t + square_ref[...] * F32(1.0 / width)
        rate = STEP / (jnp.sqrt(new_acc) + EPS)
        loads[t].wait()
        for block in range(rows // 128):
            at = slice(block * 128, (block + 1) * 128)
            lane_at = block * tables + t
            out_ref[t, at, :] = out_ref[t, at, :] - sum_ref[at, :] * rate[:, lane_at : lane_at + 1]
            if t == tables - 1 and block == 3:
                send_all(
                    lambda p: part_ref.at[pl.ds(0, 1)],
                    lambda slot: parts_ref.at[slot],
                    tables + 1,
                )
    nacc_ref[...] = (acc_t + square_ref[...] * F32(1.0 / width)).T
    parts_ref[pl.ds(peers - 1, 1)] = part_ref[0:1].reshape(1, 1, 128)
    pltpu.make_async_copy(
        parts_ref.at[others], parts_ref.at[others], recv_sem.at[tables + 1]
    ).wait()
    total = jnp.sum(parts_ref[...].reshape(peers, 128), axis=0, keepdims=True)
    total = jnp.sum(total, axis=1, keepdims=True)
    scale_ref[...] = jnp.broadcast_to(jnp.sqrt(total * F32(1.0 / count)), scale_ref.shape)
    for t in range(tables):
        pltpu.make_async_copy(
            send_ref.at[t, others], send_ref.at[t, others], send_sem.at[t]
        ).wait()
    pltpu.make_async_copy(
        srow_ref.at[others], srow_ref.at[others], send_sem.at[tables]
    ).wait()
    pltpu.make_async_copy(
        parts_ref.at[others], parts_ref.at[others], send_sem.at[tables + 1]
    ).wait()


def write_out(tab_ref, acc_ref, scale_ref, out_ref, nacc_ref, total_ref, sem):
    tables = tab_ref.shape[0]
    stores = [
        pltpu.make_async_copy(tab_ref.at[t], out_ref.at[t], sem.at[t]) for t in range(tables)
    ]
    for store in stores:
        store.start()
    nacc_ref[...] = acc_ref[...]
    total_ref[...] = scale_ref[0:1, 0:1]
    for store in stores:
        store.wait()


def per_device(peers, sizes, lookup_ids, bag_lengths, pooled_gradients, tables, accumulators):
    samples, count_tables, bag_width = lookup_ids.shape
    width = pooled_gradients.shape[2]
    rows_dev = tables.shape[1]
    lookups = samples * bag_width
    bucket = lookups // peers
    blocks = rows_dev // 128
    count = width * count_tables * lookups * peers
    in_vmem = pl.BlockSpec(memory_space=VMEM)
    in_any = pl.BlockSpec(memory_space=pl.ANY)
    in_hbm = pl.BlockSpec(memory_space=pltpu.HBM)
    acc = accumulators.reshape(count_tables, blocks, 128).transpose(1, 0, 2).reshape(-1, 128)
    moved, new_acc, scale = pl.pallas_call(
        functools.partial(
            exchange_and_update, sizes, 37, rows_dev.bit_length() - 1, bucket, count
        ),
        out_shape=(
            VMEM(tables.shape, F32),
            VMEM(acc.shape, F32),
            VMEM((8, 128), F32),
        ),
        in_specs=[in_hbm] * 5,
        out_specs=(in_vmem, in_vmem, in_vmem),
        scratch_shapes=[
            VMEM((count_tables, bag_width, samples), I32),
            VMEM((count_tables, samples), I32),
            VMEM((samples * count_tables, width), BF16),
            VMEM(acc.shape, F32),
            VMEM((count_tables, peers, bucket, width), BF16),
            VMEM((peers, 1, 128), I32),
            VMEM((count_tables, peers, bucket, width), BF16),
            VMEM((peers, 1, 128), I32),
            VMEM((samples * count_tables, width), F32),
            VMEM((count_tables, samples, width), BF16),
            VMEM((peers * bucket, width), F32),
            VMEM((rows_dev, width), F32),
            VMEM((256, lookups), BF16),
            VMEM((16, lookups), BF16),
            VMEM((lookups, 2 * width), BF16),
            VMEM((128, 128), F32),
            VMEM((8, 128), F32),
            VMEM((peers, 1, 128), F32),
            pltpu.SemaphoreType.DMA((count_tables + 4,)),
            pltpu.SemaphoreType.DMA((count_tables + 2,)),
            pltpu.SemaphoreType.DMA((count_tables + 2,)),
        ],
        compiler_params=pltpu.CompilerParams(
            collective_id=0, has_side_effects=True, vmem_limit_bytes=58_585_088
        ),
        name="exchange",
    )(
        lookup_ids.transpose(1, 2, 0),
        bag_lengths.T,
        pooled_gradients.reshape(samples * count_tables, width),
        acc,
        tables,
    )
    new_tables, new_acc, total = pl.pallas_call(
        write_out,
        out_shape=(
            jax.ShapeDtypeStruct(tables.shape, F32),
            jax.ShapeDtypeStruct(acc.shape, F32),
            jax.ShapeDtypeStruct((1, 1), F32),
        ),
        in_specs=[in_vmem] * 3,
        out_specs=(in_any, in_vmem, in_vmem),
        scratch_shapes=[pltpu.SemaphoreType.DMA((count_tables,))],
        compiler_params=pltpu.CompilerParams(vmem_limit_bytes=16 * 2**20),
        name="write_out",
    )(moved, new_acc, scale)
    new_acc = new_acc.reshape(blocks, count_tables, 128).transpose(1, 0, 2).reshape(accumulators.shape)
    return (new_tables, new_acc, total[0, 0])


def solution(mesh):
    peers = mesh.devices.size
    return jax.shard_map(
        functools.partial(per_device, peers, (4, 4, 4, 2)),
        mesh=mesh,
        in_specs=(
            P("shard", None, None),
            P("shard", None),
            P("shard", None, None),
            P(None, "shard", None),
            P(None, "shard"),
        ),
        out_specs=(P(None, "shard", None), P(None, "shard"), P()),
        check_vma=False,
    )
```

```python
import functools

import jax
import jax.numpy as jnp
from jax import lax
from jax.experimental import pallas as pl
from jax.experimental.pallas import tpu as pltpu
from jax.sharding import PartitionSpec as P

STEP = 0.5
EPS = 1e-08
F32 = jnp.float32
BF16 = jnp.bfloat16
I32 = jnp.int32
MESH = pl.DeviceIdType.MESH
VMEM = pltpu.VMEM


def iota(shape, dim):
    return lax.broadcasted_iota(I32, shape, dim)


def one_if(mask):
    return jnp.where(mask, F32(1.0), F32(0.0)).astype(BF16)


def nt_dot(a, b):
    return lax.dot_general(a, b, (((1,), (1,)), ((), ())), preferred_element_type=F32)


def send_order(sizes):
    peers = 1
    for size in sizes:
        peers *= size
    even = []
    for k in range(peers - 1):
        rest = (37 * k) % (peers - 1) + 1
        offset = []
        for size in reversed(sizes):
            offset.insert(0, rest % size)
            rest //= size
        even.append(tuple(offset))

    def hops(offset):
        return sum(min(d, size - d) for d, size in zip(offset[:-1], sizes))

    far = sorted(even, key=lambda offset: -hops(offset))
    return far, [far.index(offset) for offset in even]


def rank_table(t, ids_ref, len_ref, peers, shift, bucket):
    bags = ids_ref.shape[2]
    width = ids_ref.shape[1]
    lens = len_ref[t : t + 1, :]
    owner_iota = iota((peers, bags), 0)
    bag_iota = iota((1, bags), 1).astype(F32)
    upper = one_if(iota((bags, bags), 0) < iota((bags, bags), 1))
    ones = jnp.ones((bags, bags), BF16)
    prefix_rhs = jnp.concatenate([upper, ones], axis=0)
    rank_iota = iota((bucket, bags), 0).astype(F32)
    seen = jnp.zeros((peers, bags), F32)
    owned = []
    values = []
    for l in range(width):
        ids = ids_ref[t, l : l + 1, :]
        owner = lax.shift_right_logical(ids, shift)
        local = lax.bitwise_and(ids, (1 << shift) - 1)
        own32 = jnp.where(owner == owner_iota, F32(1.0), F32(0.0))
        own = own32.astype(BF16)
        before = jnp.dot(
            jnp.concatenate([own, seen.astype(BF16)], axis=1),
            prefix_rhs,
            preferred_element_type=F32,
        )
        rank = jnp.sum(own32 * before, axis=0, keepdims=True)
        seen = seen + own32
        at_rank = rank == rank_iota
        bag = jnp.where(l < lens, bag_iota, F32(bags))
        high = lax.shift_right_logical(local, 6).astype(F32)
        low = lax.bitwise_and(local, 63).astype(F32)
        zero = jnp.zeros_like(rank_iota)
        values.append(
            jnp.concatenate(
                [
                    jnp.where(at_rank, bag, zero),
                    jnp.where(at_rank, high, zero),
                    jnp.where(at_rank, low, zero),
                ],
                axis=0,
            ).astype(BF16)
        )
        owned.append(own)
    table = nt_dot(jnp.concatenate(owned, axis=1), jnp.concatenate(values, axis=1))
    rows = (table[:, bucket : 2 * bucket] * 64.0 + table[:, 2 * bucket :]).astype(I32)
    return table[:, :bucket], rows


def select_table(t, bag_of, scaled_ref, send_ref, rows32_ref):
    peers, bucket = bag_of.shape
    bags = scaled_ref.shape[1]
    lane = iota((peers, bags), 1).astype(F32)
    select = jnp.concatenate([one_if(bag_of[:, r : r + 1] == lane) for r in range(bucket)], axis=0)
    moved = jnp.dot(select, scaled_ref[t], preferred_element_type=F32)
    for r in range(bucket):
        rows32_ref[pl.ds(r, peers, stride=bucket), :] = moved[r * peers : (r + 1) * peers]
    send_ref[t] = rows32_ref[...].reshape(peers, bucket, -1).astype(BF16)


def exchange_and_update(
    sizes,
    shift,
    bucket,
    count,
    ids_hbm,
    len_hbm,
    g_hbm,
    acc_hbm,
    tab_ref,
    out_ref,
    nacc_ref,
    scale_ref,
    ids_ref,
    len_ref,
    g_ref,
    acc_ref,
    send_ref,
    srow_ref,
    got_ref,
    grow_ref,
    g32_ref,
    scaled_ref,
    rows32_ref,
    sum_ref,
    low_ref,
    hot_ref,
    rhs_ref,
    square_ref,
    part_ref,
    parts_ref,
    in_sem,
    send_sem,
    recv_sem,
):
    tables, rows, width = tab_ref.shape
    bags = ids_ref.shape[2]
    peers = send_ref.shape[1]
    lookups = peers * bucket
    group = 256 // bucket
    chunks = peers // group
    half = rows // 2
    tiles = half // 256
    me = lax.axis_index("shard")
    loads = [
        pltpu.make_async_copy(tab_ref.at[t], out_ref.at[t], in_sem.at[t]) for t in range(tables)
    ]
    small = [
        pltpu.make_async_copy(src, dst, in_sem.at[tables + i])
        for i, (src, dst) in enumerate(
            ((ids_hbm, ids_ref), (len_hbm, len_ref), (g_hbm, g_ref), (acc_hbm, acc_ref))
        )
    ]
    for load in small + loads:
        load.start()
    near = []
    span = peers
    for size in sizes:
        span //= size
        here = lax.rem(lax.div(me, span), size)
        near.append([lax.rem(here + d, size) * span for d in range(size)])
    far, even = send_order(sizes)

    def peer_at(slot):
        return sum(spots[d] for spots, d in zip(near, far[slot]))

    barrier = pltpu.get_barrier_semaphore()
    for slot in range(peers - 1):
        pl.semaphore_signal(barrier, inc=1, device_id=(peer_at(slot),), device_id_type=MESH)
    for load in small:
        load.wait()

    g32_ref[...] = g_ref[...].astype(F32)
    lens = len_ref[...].astype(F32)
    lens_t = jnp.concatenate([lens, jnp.ones((128 - tables, bags), F32)], axis=0).T
    for t in range(tables):
        part = g32_ref[pl.ds(t, bags, stride=tables), :]
        scaled_ref[t] = (part / lens_t[:, t : t + 1]).astype(BF16)
    ranked = [rank_table(t, ids_ref, len_ref, peers, shift, bucket) for t in range(tables)]
    srow_ref[...] = jnp.concatenate(
        [r for _, r in ranked] + [jnp.zeros((peers, 128 - tables * bucket), I32)], axis=1
    ).reshape(srow_ref.shape)

    def send_all(src, dst, s, slots=range(peers - 1)):
        for slot in slots:
            p = peer_at(slot)
            pltpu.make_async_remote_copy(
                src_ref=src(p),
                dst_ref=dst(slot),
                send_sem=send_sem.at[s],
                recv_sem=recv_sem.at[s],
                device_id=(p,),
                device_id_type=MESH,
            ).start()

    last = tables - 1
    rows_sem = tables
    parts_sem = tables + 1
    tail = [(0, chunks // 2), (chunks // 2, 3 * chunks // 4), (3 * chunks // 4, chunks)]
    tail_sems = [last, tables + 2, tables + 3]

    def send_table(t):
        def src(p):
            return send_ref.at[t, p]

        def dst(slot):
            return got_ref.at[t, slot]

        if t < last:
            send_all(src, dst, t, even)
        else:
            for (c0, c1), s in zip(tail, tail_sems):
                send_all(src, dst, s, range(c0 * group, min(c1 * group, peers - 1)))

    def wait_for(ref, s, begin, end):
        part = ref.at[pl.ds(begin, end - begin)]
        pltpu.make_async_copy(part, part, s).wait()


    select_table(0, ranked[0][0], scaled_ref, send_ref, rows32_ref)
    select_table(1, ranked[1][0], scaled_ref, send_ref, rows32_ref)
    pl.semaphore_wait(barrier, peers - 1)
    send_table(0)
    send_all(lambda p: srow_ref.at[p], lambda slot: grow_ref.at[slot], rows_sem, even)
    for t in range(2, tables):
        select_table(t, ranked[t][0], scaled_ref, send_ref, rows32_ref)
        send_table(t - 1)
    grow_ref[pl.ds(peers - 1, 1)] = srow_ref[pl.ds(me, 1)]
    for t in range(tables):
        got_ref[t, pl.ds(peers - 1, 1)] = send_ref[t, pl.ds(me, 1)]
    send_table(tables - 1)
    acc_t = acc_ref[...].T
    square_ref[...] = jnp.zeros_like(square_ref)

    wait_for(grow_ref, recv_sem.at[rows_sem], 0, peers - 1)
    got_rows = grow_ref[...].reshape(peers, 128)
    upper = lax.shift_right_logical(got_rows, half.bit_length() - 1)
    tile = lax.shift_right_logical(lax.bitwise_and(got_rows, half - 1), 8)
    low = lax.bitwise_and(got_rows, 255)
    spread_lane = iota((128, 256 * tables), 1)
    spread = one_if(
        iota((128, 256 * tables), 0)
        == lax.shift_right_logical(spread_lane, 8) * bucket
        + lax.bitwise_and(spread_lane, bucket - 1)
    )
    lane = iota((peers, 256 * tables), 1)
    own_lane = lax.shift_right_logical(
        lax.bitwise_and(lane, 255), bucket.bit_length() - 1
    ) == lax.bitwise_and(iota((peers, 256 * tables), 0), group - 1)

    def lane_vectors(digit):
        wide = jnp.dot(digit.astype(BF16), spread, preferred_element_type=F32)
        wide = jnp.where(own_lane, wide, F32(0.0)).reshape(chunks, group, 256 * tables)
        return jnp.sum(wide, axis=1)

    lows = lane_vectors(low)
    tiles_of = lane_vectors(tile)
    uppers = lane_vectors(upper)
    upper_t = jnp.concatenate(
        [uppers[:, i * 128 : (i + 1) * 128] for i in range(2 * tables)]
        + [jnp.zeros((128 - 2 * tables * chunks, 128), F32)],
        axis=0,
    ).T
    lane_id = iota((128, 128), 1)
    sub_id = iota((256, 256), 0).astype(F32)

    for t in range(tables):
        for c in range(chunks):
            col = slice(c * 256, (c + 1) * 256)
            low_ref[:, col] = one_if(lows[c : c + 1, t * 256 : (t + 1) * 256] == sub_id)
            hot_ref[:, col] = jnp.broadcast_to(
                tiles_of[c : c + 1, t * 256 : (t + 1) * 256], (16, 256)
            ).astype(BF16)

        def add_chunks(c0, c1, t=t):
            for c in range(c0, c1):
                for h in range(2):
                    k = 2 * t + h
                    is_upper = upper_t[:, k * chunks + c : k * chunks + c + 1]
                    src = slice(c * group + h * group // 2, c * group + (h + 1) * group // 2)
                    terms = got_ref[t, src].reshape(128, width)
                    up = jnp.broadcast_to(is_upper, (128, width)).astype(BF16)
                    row = slice(c * 256 + h * 128, c * 256 + (h + 1) * 128)
                    rhs_ref[row, width:] = terms * up
                    rhs_ref[row, :width] = terms * (BF16(1.0) - up)
            depth = (c1 - c0) * 256
            span = slice(c0 * 256, c1 * 256)

            def tile_step(m, carry):
                hot = hot_ref[:, span]
                mask = jnp.where(hot == m.astype(F32).astype(BF16), BF16(1.0), BF16(0.0))
                lhs = (low_ref[:, span].reshape(16, 16, depth) * mask[None]).reshape(256, depth)
                both = jnp.dot(lhs, rhs_ref[span, :], preferred_element_type=F32)
                for p in range(2):
                    for h in range(2):
                        s = both[h * 128 : (h + 1) * 128, p * width : (p + 1) * width]
                        block = p * (half // 128) + 2 * m + h
                        at = pl.ds(pl.multiple_of(block * 128, 128), 128)
                        if c0 > 0:
                            s = s + sum_ref[at, :]
                        sum_ref[at, :] = s
                        if c1 == chunks:
                            squares = jnp.sum(s * s, axis=1, keepdims=True)
                            square_ref[...] = jnp.where(
                                lane_id == block * tables + t, squares, square_ref[...]
                            )
                return carry

            lax.fori_loop(0, tiles, tile_step, 0, unroll=2 if depth > 1024 else 4)

        if t < last:
            wait_for(got_ref.at[t], recv_sem.at[t], 0, peers - 1)
            add_chunks(0, chunks)
        else:
            for (c0, c1), s in zip(tail, tail_sems):
                wait_for(got_ref.at[t], recv_sem.at[s], c0 * group, min(c1 * group, peers - 1))
                add_chunks(c0, c1)
        if t == tables - 1:
            part_ref[...] = jnp.broadcast_to(
                jnp.sum(square_ref[...], axis=0, keepdims=True), part_ref.shape
            )
        new_acc = acc_t + square_ref[...] * F32(1.0 / width)
        rate = STEP / (jnp.sqrt(new_acc) + EPS)
        loads[t].wait()
        for block in range(rows // 128):
            at = slice(block * 128, (block + 1) * 128)
            lane_at = block * tables + t
            out_ref[t, at, :] = out_ref[t, at, :] - sum_ref[at, :] * rate[:, lane_at : lane_at + 1]
            if t == tables - 1 and block == 3:
                send_all(
                    lambda p: part_ref.at[pl.ds(0, 1)],
                    lambda slot: parts_ref.at[slot],
                    parts_sem,
                )
    nacc_ref[...] = (acc_t + square_ref[...] * F32(1.0 / width)).T
    parts_ref[pl.ds(peers - 1, 1)] = part_ref[0:1].reshape(1, 1, 128)
    wait_for(parts_ref, recv_sem.at[parts_sem], 0, peers - 1)
    total = jnp.sum(parts_ref[...].reshape(peers, 128), axis=0, keepdims=True)
    total = jnp.sum(total, axis=1, keepdims=True)
    scale_ref[...] = jnp.broadcast_to(jnp.sqrt(total * F32(1.0 / count)), scale_ref.shape)
    for t in range(last):
        wait_for(send_ref.at[t], send_sem.at[t], 0, peers - 1)
    for (c0, c1), s in zip(tail, tail_sems):
        wait_for(send_ref.at[last], send_sem.at[s], c0 * group, min(c1 * group, peers - 1))
    wait_for(srow_ref, send_sem.at[rows_sem], 0, peers - 1)
    wait_for(parts_ref, send_sem.at[parts_sem], 0, peers - 1)


def write_out(tab_ref, acc_ref, scale_ref, out_ref, nacc_ref, total_ref, sem):
    tables, rows, _ = tab_ref.shape
    stores = [pltpu.make_async_copy(acc_ref, nacc_ref, sem.at[2 * tables])]
    for t in range(tables):
        for h in range(2):
            part = pl.ds(h * rows // 2, rows // 2)
            stores.append(
                pltpu.make_async_copy(
                    tab_ref.at[t, part], out_ref.at[t, part], sem.at[2 * t + h]
                )
            )
    for store in stores:
        store.start()
    total_ref[...] = scale_ref[0:1, 0:1]
    for store in stores:
        store.wait()


def per_device(peers, sizes, lookup_ids, bag_lengths, pooled_gradients, tables, accumulators):
    samples, count_tables, bag_width = lookup_ids.shape
    width = pooled_gradients.shape[2]
    rows_dev = tables.shape[1]
    lookups = samples * bag_width
    bucket = lookups // peers
    blocks = rows_dev // 128
    count = width * count_tables * lookups * peers
    in_vmem = pl.BlockSpec(memory_space=VMEM)
    in_any = pl.BlockSpec(memory_space=pl.ANY)
    in_hbm = pl.BlockSpec(memory_space=pltpu.HBM)
    acc = accumulators.reshape(count_tables, blocks, 128).transpose(1, 0, 2).reshape(-1, 128)
    moved, new_acc, scale = pl.pallas_call(
        functools.partial(
            exchange_and_update, sizes, rows_dev.bit_length() - 1, bucket, count
        ),
        out_shape=(
            VMEM(tables.shape, F32),
            VMEM(acc.shape, F32),
            VMEM((8, 128), F32),
        ),
        in_specs=[in_hbm] * 5,
        out_specs=(in_vmem, in_vmem, in_vmem),
        scratch_shapes=[
            VMEM((count_tables, bag_width, samples), I32),
            VMEM((count_tables, samples), I32),
            VMEM((samples * count_tables, width), BF16),
            VMEM(acc.shape, F32),
            VMEM((count_tables, peers, bucket, width), BF16),
            VMEM((peers, 1, 128), I32),
            VMEM((count_tables, peers, bucket, width), BF16),
            VMEM((peers, 1, 128), I32),
            VMEM((samples * count_tables, width), F32),
            VMEM((count_tables, samples, width), BF16),
            VMEM((peers * bucket, width), F32),
            VMEM((rows_dev, width), F32),
            VMEM((256, lookups), BF16),
            VMEM((16, lookups), BF16),
            VMEM((lookups, 2 * width), BF16),
            VMEM((128, 128), F32),
            VMEM((8, 128), F32),
            VMEM((peers, 1, 128), F32),
            pltpu.SemaphoreType.DMA((count_tables + 4,)),
            pltpu.SemaphoreType.DMA((count_tables + 4,)),
            pltpu.SemaphoreType.DMA((count_tables + 4,)),
        ],
        compiler_params=pltpu.CompilerParams(
            collective_id=0, has_side_effects=True, vmem_limit_bytes=58_585_088
        ),
        name="exchange",
    )(
        lookup_ids.transpose(1, 2, 0),
        bag_lengths.T,
        pooled_gradients.reshape(samples * count_tables, width),
        acc,
        tables,
    )
    new_tables, new_acc, total = pl.pallas_call(
        write_out,
        out_shape=(
            jax.ShapeDtypeStruct(tables.shape, F32),
            jax.ShapeDtypeStruct(acc.shape, F32),
            jax.ShapeDtypeStruct((1, 1), F32),
        ),
        in_specs=[in_vmem] * 3,
        out_specs=(in_any, in_any, in_vmem),
        scratch_shapes=[pltpu.SemaphoreType.DMA((2 * count_tables + 1,))],
        compiler_params=pltpu.CompilerParams(vmem_limit_bytes=16 * 2**20),
        name="write_out",
    )(moved, new_acc, scale)
    new_acc = new_acc.reshape(blocks, count_tables, 128).transpose(1, 0, 2).reshape(accumulators.shape)
    return (new_tables, new_acc, total[0, 0])


def solution(mesh):
    peers = mesh.devices.size
    return jax.shard_map(
        functools.partial(per_device, peers, (4, 4, 4, 2)),
        mesh=mesh,
        in_specs=(
            P("shard", None, None),
            P("shard", None),
            P("shard", None, None),
            P(None, "shard", None),
            P(None, "shard"),
        ),
        out_specs=(P(None, "shard", None), P(None, "shard"), P()),
        check_vma=False,
    )
```

```python
import functools

import jax
import jax.numpy as jnp
from jax import lax
from jax.experimental import pallas as pl
from jax.experimental.pallas import tpu as pltpu
from jax.sharding import PartitionSpec as P

STEP = 0.5
EPS = 1e-08
F32 = jnp.float32
BF16 = jnp.bfloat16
I32 = jnp.int32
MESH = pl.DeviceIdType.MESH
VMEM = pltpu.VMEM


def iota(shape, dim):
    return lax.broadcasted_iota(I32, shape, dim)


def one_if(mask):
    return jnp.where(mask, F32(1.0), F32(0.0)).astype(BF16)


def nt_dot(a, b):
    return lax.dot_general(a, b, (((1,), (1,)), ((), ())), preferred_element_type=F32)


EVEN = 2
WIDE = 4
UNROLL = 1


def send_order(sizes):
    peers = 1
    for size in sizes:
        peers *= size
    even = []
    for k in range(peers - 1):
        rest = (37 * k) % (peers - 1) + 1
        offset = []
        for size in reversed(sizes):
            offset.insert(0, rest % size)
            rest //= size
        even.append(tuple(offset))

    def hops(offset):
        return sum(min(d, size - d) for d, size in zip(offset[:-1], sizes))

    far = sorted(even, key=lambda offset: -hops(offset))
    return far, [far.index(offset) for offset in even]


def rank_table(t, ids_ref, len_ref, peers, shift, bucket):
    bags = ids_ref.shape[2]
    width = ids_ref.shape[1]
    lens = len_ref[t : t + 1, :]
    owner_iota = iota((peers, bags), 0)
    bag_iota = iota((1, bags), 1).astype(F32)
    upper = one_if(iota((bags, bags), 0) < iota((bags, bags), 1))
    ones = jnp.ones((bags, bags), BF16)
    prefix_rhs = jnp.concatenate([upper, ones], axis=0)
    rank_iota = iota((bucket, bags), 0).astype(F32)
    seen = jnp.zeros((peers, bags), F32)
    owned = []
    values = []
    for l in range(width):
        ids = ids_ref[t, l : l + 1, :]
        owner = lax.shift_right_logical(ids, shift)
        local = lax.bitwise_and(ids, (1 << shift) - 1)
        own32 = jnp.where(owner == owner_iota, F32(1.0), F32(0.0))
        own = own32.astype(BF16)
        before = jnp.dot(
            jnp.concatenate([own, seen.astype(BF16)], axis=1),
            prefix_rhs,
            preferred_element_type=F32,
        )
        rank = jnp.sum(own32 * before, axis=0, keepdims=True)
        seen = seen + own32
        at_rank = rank == rank_iota
        bag = jnp.where(l < lens, bag_iota, F32(bags))
        high = lax.shift_right_logical(local, 6).astype(F32)
        low = lax.bitwise_and(local, 63).astype(F32)
        zero = jnp.zeros_like(rank_iota)
        values.append(
            jnp.concatenate(
                [
                    jnp.where(at_rank, bag, zero),
                    jnp.where(at_rank, high, zero),
                    jnp.where(at_rank, low, zero),
                ],
                axis=0,
            ).astype(BF16)
        )
        owned.append(own)
    table = nt_dot(jnp.concatenate(owned, axis=1), jnp.concatenate(values, axis=1))
    rows = (table[:, bucket : 2 * bucket] * 64.0 + table[:, 2 * bucket :]).astype(I32)
    return table[:, :bucket], rows


def select_table(t, bag_of, scaled_ref, send_ref, rows32_ref):
    peers, bucket = bag_of.shape
    bags = scaled_ref.shape[1]
    lane = iota((peers, bags), 1).astype(F32)
    select = jnp.concatenate([one_if(bag_of[:, r : r + 1] == lane) for r in range(bucket)], axis=0)
    moved = jnp.dot(select, scaled_ref[t], preferred_element_type=F32)
    for r in range(bucket):
        rows32_ref[pl.ds(r, peers, stride=bucket), :] = moved[r * peers : (r + 1) * peers]
    send_ref[t] = rows32_ref[...].reshape(peers, bucket, -1).astype(BF16)


def exchange_and_update(
    sizes,
    shift,
    bucket,
    count,
    ids_hbm,
    len_hbm,
    g_hbm,
    acc_hbm,
    tab_ref,
    out_ref,
    nacc_ref,
    scale_ref,
    ids_ref,
    len_ref,
    g_ref,
    acc_ref,
    send_ref,
    srow_ref,
    got_ref,
    grow_ref,
    g32_ref,
    scaled_ref,
    rows32_ref,
    sum_ref,
    low_ref,
    hot_ref,
    rhs_ref,
    square_ref,
    part_ref,
    parts_ref,
    in_sem,
    send_sem,
    recv_sem,
):
    tables, rows, width = tab_ref.shape
    bags = ids_ref.shape[2]
    peers = send_ref.shape[1]
    lookups = peers * bucket
    group = 256 // bucket
    chunks = peers // group
    half = rows // 2
    tiles = half // 256
    me = lax.axis_index("shard")
    loads = [
        pltpu.make_async_copy(tab_ref.at[t], out_ref.at[t], in_sem.at[t]) for t in range(tables)
    ]
    small = [
        pltpu.make_async_copy(src, dst, in_sem.at[tables + i])
        for i, (src, dst) in enumerate(
            ((ids_hbm, ids_ref), (len_hbm, len_ref), (g_hbm, g_ref), (acc_hbm, acc_ref))
        )
    ]
    for load in small + loads:
        load.start()
    near = []
    span = peers
    for size in sizes:
        span //= size
        here = lax.rem(lax.div(me, span), size)
        near.append([lax.rem(here + d, size) * span for d in range(size)])
    far, even = send_order(sizes)

    def peer_at(slot):
        return sum(spots[d] for spots, d in zip(near, far[slot]))

    barrier = pltpu.get_barrier_semaphore()
    for slot in range(peers - 1):
        pl.semaphore_signal(barrier, inc=1, device_id=(peer_at(slot),), device_id_type=MESH)
    for load in small:
        load.wait()

    g32_ref[...] = g_ref[...].astype(F32)
    lens = len_ref[...].astype(F32)
    lens_t = jnp.concatenate([lens, jnp.ones((128 - tables, bags), F32)], axis=0).T
    for t in range(tables):
        part = g32_ref[pl.ds(t, bags, stride=tables), :]
        scaled_ref[t] = (part / lens_t[:, t : t + 1]).astype(BF16)
    ranked = [rank_table(t, ids_ref, len_ref, peers, shift, bucket) for t in range(tables)]
    srow_ref[...] = jnp.concatenate(
        [r for _, r in ranked] + [jnp.zeros((peers, 128 - tables * bucket), I32)], axis=1
    ).reshape(srow_ref.shape)

    def send(p, src, dst, s):
        pltpu.make_async_remote_copy(
            src_ref=src,
            dst_ref=dst,
            send_sem=send_sem.at[s],
            recv_sem=recv_sem.at[s],
            device_id=(p,),
            device_id_type=MESH,
        ).start()

    last = tables - 1
    rows_sem = tables
    parts_sem = tables + 1
    tail = [(0, chunks // 2), (chunks // 2, 3 * chunks // 4), (3 * chunks // 4, chunks)]
    tail_sems = [last, tables + 2, tables + 3]

    def send_table(t):
        for slot in even if t < EVEN else range(peers - 1):
            p = peer_at(slot)
            if t == 0:
                send(p, srow_ref.at[p], grow_ref.at[slot], rows_sem)
            sem = t
            if t == last:
                sem = next(s for (_, c1), s in zip(tail, tail_sems) if slot < c1 * group)
            send(p, send_ref.at[t, p], got_ref.at[t, slot], sem)

    def wait_for(ref, s, begin, end):
        part = ref.at[pl.ds(begin, end - begin)]
        pltpu.make_async_copy(part, part, s).wait()


    select_table(0, ranked[0][0], scaled_ref, send_ref, rows32_ref)
    select_table(1, ranked[1][0], scaled_ref, send_ref, rows32_ref)
    pl.semaphore_wait(barrier, peers - 1)
    send_table(0)
    for t in range(2, tables):
        select_table(t, ranked[t][0], scaled_ref, send_ref, rows32_ref)
        if t == 2:
            send_table(1)
    grow_ref[pl.ds(peers - 1, 1)] = srow_ref[pl.ds(me, 1)]
    for t in range(tables):
        got_ref[t, pl.ds(peers - 1, 1)] = send_ref[t, pl.ds(me, 1)]
    wait_for(send_ref.at[0], send_sem.at[0], 0, peers - 1)
    send_table(2)
    acc_t = acc_ref[...].T
    square_ref[...] = jnp.zeros_like(square_ref)

    wait_for(grow_ref, recv_sem.at[rows_sem], 0, peers - 1)
    got_rows = grow_ref[...].reshape(peers, 128)
    upper = lax.shift_right_logical(got_rows, half.bit_length() - 1)
    tile = lax.shift_right_logical(lax.bitwise_and(got_rows, half - 1), 8)
    low = lax.bitwise_and(got_rows, 255)
    spread_lane = iota((128, 256 * tables), 1)
    spread = one_if(
        iota((128, 256 * tables), 0)
        == lax.shift_right_logical(spread_lane, 8) * bucket
        + lax.bitwise_and(spread_lane, bucket - 1)
    )
    lane = iota((peers, 256 * tables), 1)
    own_lane = lax.shift_right_logical(
        lax.bitwise_and(lane, 255), bucket.bit_length() - 1
    ) == lax.bitwise_and(iota((peers, 256 * tables), 0), group - 1)

    def lane_vectors(digit):
        wide = jnp.dot(digit.astype(BF16), spread, preferred_element_type=F32)
        wide = jnp.where(own_lane, wide, F32(0.0)).reshape(chunks, group, 256 * tables)
        return jnp.sum(wide, axis=1)

    lows = lane_vectors(low)
    tiles_of = lane_vectors(tile)
    uppers = lane_vectors(upper)
    upper_t = jnp.concatenate(
        [uppers[:, i * 128 : (i + 1) * 128] for i in range(2 * tables)]
        + [jnp.zeros((128 - 2 * tables * chunks, 128), F32)],
        axis=0,
    ).T
    lane_id = iota((128, 128), 1)
    sub_id = iota((256, 256), 0).astype(F32)

    for t in range(tables):
        for c in range(chunks):
            col = slice(c * 256, (c + 1) * 256)
            low_ref[:, col] = one_if(lows[c : c + 1, t * 256 : (t + 1) * 256] == sub_id)
            hot_ref[:, col] = jnp.broadcast_to(
                tiles_of[c : c + 1, t * 256 : (t + 1) * 256], (16, 256)
            ).astype(BF16)

        def add_chunks(c0, c1, t=t):
            for c in range(c0, c1):
                for h in range(2):
                    k = 2 * t + h
                    is_upper = upper_t[:, k * chunks + c : k * chunks + c + 1]
                    src = slice(c * group + h * group // 2, c * group + (h + 1) * group // 2)
                    terms = got_ref[t, src].reshape(128, width)
                    up = jnp.broadcast_to(is_upper, (128, width)).astype(BF16)
                    row = slice(c * 256 + h * 128, c * 256 + (h + 1) * 128)
                    rhs_ref[row, width:] = terms * up
                    rhs_ref[row, :width] = terms * (BF16(1.0) - up)
            depth = (c1 - c0) * 256
            span = slice(c0 * 256, c1 * 256)

            def tile_step(m, carry):
                hot = hot_ref[:, span]
                low = low_ref[:, span].reshape(16, 16, depth)
                lhs = []
                for i in range(WIDE):
                    at_tile = hot == (WIDE * m + i).astype(F32).astype(BF16)
                    mask = jnp.where(at_tile, BF16(1.0), BF16(0.0))
                    lhs.append((low * mask[None]).reshape(256, depth))
                both = jnp.dot(
                    jnp.concatenate(lhs, axis=0), rhs_ref[span, :], preferred_element_type=F32
                )
                for p in range(2):
                    for h in range(2 * WIDE):
                        s = both[h * 128 : (h + 1) * 128, p * width : (p + 1) * width]
                        block = p * (half // 128) + 2 * WIDE * m + h
                        at = pl.ds(pl.multiple_of(block * 128, 128), 128)
                        if c0 > 0:
                            s = s + sum_ref[t, at, :]
                        sum_ref[t, at, :] = s
                        if c1 == chunks:
                            squares = jnp.sum(s * s, axis=1, keepdims=True)
                            square_ref[...] = jnp.where(
                                lane_id == block * tables + t, squares, square_ref[...]
                            )
                return carry

            lax.fori_loop(0, tiles // WIDE, tile_step, 0, unroll=UNROLL if depth > 1024 else 2)

        if t == 1:
            wait_for(send_ref.at[1], send_sem.at[1], 0, peers - 1)
            send_table(3)
        if t < last:
            wait_for(got_ref.at[t], recv_sem.at[t], 0, peers - 1)
            add_chunks(0, chunks)
        else:
            for (c0, c1), s in zip(tail, tail_sems):
                wait_for(got_ref.at[t], recv_sem.at[s], c0 * group, min(c1 * group, peers - 1))
                add_chunks(c0, c1)
    part_ref[...] = jnp.broadcast_to(
        jnp.sum(square_ref[...], axis=0, keepdims=True), part_ref.shape
    )
    new_acc = acc_t + square_ref[...] * F32(1.0 / width)
    rate = STEP / (jnp.sqrt(new_acc) + EPS)
    nacc_ref[...] = new_acc.T
    for slot in range(peers - 1):
        send(peer_at(slot), part_ref.at[pl.ds(0, 1)], parts_ref.at[slot], parts_sem)
    for t in range(tables):
        loads[t].wait()
        for block in range(rows // 128):
            at = slice(block * 128, (block + 1) * 128)
            lane_at = block * tables + t
            out_ref[t, at, :] = out_ref[t, at, :] - sum_ref[t, at, :] * rate[:, lane_at : lane_at + 1]
    parts_ref[pl.ds(peers - 1, 1)] = part_ref[0:1].reshape(1, 1, 128)
    wait_for(parts_ref, recv_sem.at[parts_sem], 0, peers - 1)
    total = jnp.sum(parts_ref[...].reshape(peers, 128), axis=0, keepdims=True)
    total = jnp.sum(total, axis=1, keepdims=True)
    scale_ref[...] = jnp.broadcast_to(jnp.sqrt(total * F32(1.0 / count)), scale_ref.shape)
    wait_for(send_ref.at[2], send_sem.at[2], 0, peers - 1)
    for (c0, c1), s in zip(tail, tail_sems):
        wait_for(send_ref.at[last], send_sem.at[s], c0 * group, min(c1 * group, peers - 1))
    wait_for(srow_ref, send_sem.at[rows_sem], 0, peers - 1)
    wait_for(parts_ref, send_sem.at[parts_sem], 0, peers - 1)


def write_out(tab_ref, acc_ref, scale_ref, out_ref, nacc_ref, total_ref, sem):
    tables, rows, _ = tab_ref.shape
    stores = [pltpu.make_async_copy(acc_ref, nacc_ref, sem.at[2 * tables])]
    for t in range(tables):
        for h in range(2):
            part = pl.ds(h * rows // 2, rows // 2)
            stores.append(
                pltpu.make_async_copy(
                    tab_ref.at[t, part], out_ref.at[t, part], sem.at[2 * t + h]
                )
            )
    for store in stores:
        store.start()
    total_ref[...] = scale_ref[0:1, 0:1]
    for store in stores:
        store.wait()


def per_device(peers, sizes, lookup_ids, bag_lengths, pooled_gradients, tables, accumulators):
    samples, count_tables, bag_width = lookup_ids.shape
    width = pooled_gradients.shape[2]
    rows_dev = tables.shape[1]
    lookups = samples * bag_width
    bucket = lookups // peers
    blocks = rows_dev // 128
    count = width * count_tables * lookups * peers
    in_vmem = pl.BlockSpec(memory_space=VMEM)
    in_any = pl.BlockSpec(memory_space=pl.ANY)
    in_hbm = pl.BlockSpec(memory_space=pltpu.HBM)
    acc = accumulators.reshape(count_tables, blocks, 128).transpose(1, 0, 2).reshape(-1, 128)
    moved, new_acc, scale = pl.pallas_call(
        functools.partial(
            exchange_and_update, sizes, rows_dev.bit_length() - 1, bucket, count
        ),
        out_shape=(
            VMEM(tables.shape, F32),
            VMEM(acc.shape, F32),
            VMEM((8, 128), F32),
        ),
        in_specs=[in_hbm] * 5,
        out_specs=(in_vmem, in_vmem, in_vmem),
        scratch_shapes=[
            VMEM((count_tables, bag_width, samples), I32),
            VMEM((count_tables, samples), I32),
            VMEM((samples * count_tables, width), BF16),
            VMEM(acc.shape, F32),
            VMEM((count_tables, peers, bucket, width), BF16),
            VMEM((peers, 1, 128), I32),
            VMEM((count_tables, peers, bucket, width), BF16),
            VMEM((peers, 1, 128), I32),
            VMEM((samples * count_tables, width), F32),
            VMEM((count_tables, samples, width), BF16),
            VMEM((peers * bucket, width), F32),
            VMEM(tables.shape, F32),
            VMEM((256, lookups), BF16),
            VMEM((16, lookups), BF16),
            VMEM((lookups, 2 * width), BF16),
            VMEM((128, 128), F32),
            VMEM((8, 128), F32),
            VMEM((peers, 1, 128), F32),
            pltpu.SemaphoreType.DMA((count_tables + 4,)),
            pltpu.SemaphoreType.DMA((count_tables + 4,)),
            pltpu.SemaphoreType.DMA((count_tables + 4,)),
        ],
        compiler_params=pltpu.CompilerParams(
            collective_id=0, has_side_effects=True, vmem_limit_bytes=58_585_088
        ),
        name="exchange",
    )(
        lookup_ids.transpose(1, 2, 0),
        bag_lengths.T,
        pooled_gradients.reshape(samples * count_tables, width),
        acc,
        tables,
    )
    new_tables, new_acc, total = pl.pallas_call(
        write_out,
        out_shape=(
            jax.ShapeDtypeStruct(tables.shape, F32),
            jax.ShapeDtypeStruct(acc.shape, F32),
            jax.ShapeDtypeStruct((1, 1), F32),
        ),
        in_specs=[in_vmem] * 3,
        out_specs=(in_any, in_any, in_vmem),
        scratch_shapes=[pltpu.SemaphoreType.DMA((2 * count_tables + 1,))],
        compiler_params=pltpu.CompilerParams(vmem_limit_bytes=16 * 2**20),
        name="write_out",
    )(moved, new_acc, scale)
    new_acc = new_acc.reshape(blocks, count_tables, 128).transpose(1, 0, 2).reshape(accumulators.shape)
    return (new_tables, new_acc, total[0, 0])


def solution(mesh):
    peers = mesh.devices.size
    return jax.shard_map(
        functools.partial(per_device, peers, (4, 4, 4, 2)),
        mesh=mesh,
        in_specs=(
            P("shard", None, None),
            P("shard", None),
            P("shard", None, None),
            P(None, "shard", None),
            P(None, "shard"),
        ),
        out_specs=(P(None, "shard", None), P(None, "shard"), P()),
        check_vma=False,
    )
```

```python
import functools

import jax
import jax.numpy as jnp
from jax import lax
from jax.experimental import pallas as pl
from jax.experimental.pallas import tpu as pltpu
from jax.sharding import PartitionSpec as P

STEP = 0.5
EPS = 1e-08
F32 = jnp.float32
BF16 = jnp.bfloat16
I32 = jnp.int32
MESH = pl.DeviceIdType.MESH
VMEM = pltpu.VMEM


def iota(shape, dim):
    return lax.broadcasted_iota(I32, shape, dim)


def one_if(mask):
    return jnp.where(mask, F32(1.0), F32(0.0)).astype(BF16)


def nt_dot(a, b):
    return lax.dot_general(a, b, (((1,), (1,)), ((), ())), preferred_element_type=F32)


EVEN = 2
WIDE = 4
UNROLL = 1


def send_order(sizes):
    peers = 1
    for size in sizes:
        peers *= size
    even = []
    for k in range(peers - 1):
        rest = (29 * k) % (peers - 1) + 1
        offset = []
        for size in reversed(sizes):
            offset.insert(0, rest % size)
            rest //= size
        even.append(tuple(offset))

    def hops(offset):
        return sum(min(d, size - d) for d, size in zip(offset[:-1], sizes))

    far = sorted(even, key=lambda offset: -hops(offset))
    return far, [far.index(offset) for offset in even]


def rank_table(t, ids_ref, len_ref, peers, shift, bucket):
    bags = ids_ref.shape[2]
    width = ids_ref.shape[1]
    lens = len_ref[t : t + 1, :]
    owner_iota = iota((peers, bags), 0)
    bag_iota = iota((1, bags), 1).astype(F32)
    upper = one_if(iota((bags, bags), 0) < iota((bags, bags), 1))
    ones = jnp.ones((bags, bags), BF16)
    prefix_rhs = jnp.concatenate([upper, ones], axis=0)
    rank_iota = iota((bucket, bags), 0).astype(F32)
    seen = jnp.zeros((peers, bags), F32)
    owned = []
    values = []
    for l in range(width):
        ids = ids_ref[t, l : l + 1, :]
        owner = lax.shift_right_logical(ids, shift)
        local = lax.bitwise_and(ids, (1 << shift) - 1)
        own32 = jnp.where(owner == owner_iota, F32(1.0), F32(0.0))
        own = own32.astype(BF16)
        before = jnp.dot(
            jnp.concatenate([own, seen.astype(BF16)], axis=1),
            prefix_rhs,
            preferred_element_type=F32,
        )
        rank = jnp.sum(own32 * before, axis=0, keepdims=True)
        seen = seen + own32
        at_rank = rank == rank_iota
        bag = jnp.where(l < lens, bag_iota, F32(bags))
        high = lax.shift_right_logical(local, 6).astype(F32)
        low = lax.bitwise_and(local, 63).astype(F32)
        zero = jnp.zeros_like(rank_iota)
        values.append(
            jnp.concatenate(
                [
                    jnp.where(at_rank, bag, zero),
                    jnp.where(at_rank, high, zero),
                    jnp.where(at_rank, low, zero),
                ],
                axis=0,
            ).astype(BF16)
        )
        owned.append(own)
    table = nt_dot(jnp.concatenate(owned, axis=1), jnp.concatenate(values, axis=1))
    rows = (table[:, bucket : 2 * bucket] * 64.0 + table[:, 2 * bucket :]).astype(I32)
    return table[:, :bucket], rows


def select_table(t, bag_of, scaled_ref, send_ref, rows32_ref):
    peers, bucket = bag_of.shape
    bags = scaled_ref.shape[1]
    lane = iota((peers, bags), 1).astype(F32)
    select = jnp.concatenate([one_if(bag_of[:, r : r + 1] == lane) for r in range(bucket)], axis=0)
    moved = jnp.dot(select, scaled_ref[t], preferred_element_type=F32)
    for r in range(bucket):
        rows32_ref[pl.ds(r, peers, stride=bucket), :] = moved[r * peers : (r + 1) * peers]
    send_ref[t] = rows32_ref[...].reshape(peers, bucket, -1).astype(BF16)


def exchange_and_update(
    sizes,
    shift,
    bucket,
    count,
    ids_hbm,
    len_hbm,
    g_hbm,
    acc_hbm,
    tab_ref,
    out_ref,
    nacc_ref,
    scale_ref,
    ids_ref,
    len_ref,
    g_ref,
    acc_ref,
    send_ref,
    srow_ref,
    got_ref,
    grow_ref,
    g32_ref,
    scaled_ref,
    rows32_ref,
    sum_ref,
    low_ref,
    hot_ref,
    rhs_ref,
    square_ref,
    part_ref,
    parts_ref,
    in_sem,
    send_sem,
    recv_sem,
):
    tables, rows, width = tab_ref.shape
    bags = ids_ref.shape[2]
    peers = send_ref.shape[1]
    lookups = peers * bucket
    group = 256 // bucket
    chunks = peers // group
    half = rows // 2
    tiles = half // 256
    me = lax.axis_index("shard")
    loads = [
        pltpu.make_async_copy(tab_ref.at[t], out_ref.at[t], in_sem.at[t]) for t in range(tables)
    ]
    small = [
        pltpu.make_async_copy(src, dst, in_sem.at[tables + i])
        for i, (src, dst) in enumerate(
            ((ids_hbm, ids_ref), (len_hbm, len_ref), (g_hbm, g_ref), (acc_hbm, acc_ref))
        )
    ]
    for load in small + loads:
        load.start()
    near = []
    span = peers
    for size in sizes:
        span //= size
        here = lax.rem(lax.div(me, span), size)
        near.append([lax.rem(here + d, size) * span for d in range(size)])
    far, even = send_order(sizes)

    def peer_at(slot):
        return sum(spots[d] for spots, d in zip(near, far[slot]))

    barrier = pltpu.get_barrier_semaphore()
    for slot in range(peers - 1):
        pl.semaphore_signal(barrier, inc=1, device_id=(peer_at(slot),), device_id_type=MESH)
    for load in small:
        load.wait()

    g32_ref[...] = g_ref[...].astype(F32)
    lens = len_ref[...].astype(F32)
    lens_t = jnp.concatenate([lens, jnp.ones((128 - tables, bags), F32)], axis=0).T
    for t in range(tables):
        part = g32_ref[pl.ds(t, bags, stride=tables), :]
        scaled_ref[t] = (part / lens_t[:, t : t + 1]).astype(BF16)
    ranked = [rank_table(t, ids_ref, len_ref, peers, shift, bucket) for t in range(tables)]
    srow_ref[...] = jnp.concatenate(
        [r for _, r in ranked] + [jnp.zeros((peers, 128 - tables * bucket), I32)], axis=1
    ).reshape(srow_ref.shape)

    def send(p, src, dst, s):
        pltpu.make_async_remote_copy(
            src_ref=src,
            dst_ref=dst,
            send_sem=send_sem.at[s],
            recv_sem=recv_sem.at[s],
            device_id=(p,),
            device_id_type=MESH,
        ).start()

    last = tables - 1
    rows_sem = tables
    parts_sem = tables + 1
    tail = [(0, chunks // 2), (chunks // 2, chunks)]
    tail_sems = [last, tables + 2]

    def send_table(t):
        for slot in even if t < EVEN else range(peers - 1):
            p = peer_at(slot)
            if t == 0:
                send(p, srow_ref.at[p], grow_ref.at[slot], rows_sem)
            sem = t
            if t == last:
                sem = next(s for (_, c1), s in zip(tail, tail_sems) if slot < c1 * group)
            send(p, send_ref.at[t, p], got_ref.at[t, slot], sem)

    def wait_for(ref, s, begin, end):
        part = ref.at[pl.ds(begin, end - begin)]
        pltpu.make_async_copy(part, part, s).wait()


    select_table(0, ranked[0][0], scaled_ref, send_ref, rows32_ref)
    select_table(1, ranked[1][0], scaled_ref, send_ref, rows32_ref)
    pl.semaphore_wait(barrier, peers - 1)
    send_table(0)
    for t in range(2, tables):
        select_table(t, ranked[t][0], scaled_ref, send_ref, rows32_ref)
        if t == 2:
            send_table(1)
    grow_ref[pl.ds(peers - 1, 1)] = srow_ref[pl.ds(me, 1)]
    for t in range(tables):
        got_ref[t, pl.ds(peers - 1, 1)] = send_ref[t, pl.ds(me, 1)]
    wait_for(send_ref.at[0], send_sem.at[0], 0, peers - 1)
    send_table(2)
    acc_t = acc_ref[...].T
    square_ref[...] = jnp.zeros_like(square_ref)

    wait_for(grow_ref, recv_sem.at[rows_sem], 0, peers - 1)
    got_rows = grow_ref[...].reshape(peers, 128)
    upper = lax.shift_right_logical(got_rows, half.bit_length() - 1)
    tile = lax.shift_right_logical(lax.bitwise_and(got_rows, half - 1), 8)
    low = lax.bitwise_and(got_rows, 255)
    spread_lane = iota((128, 256 * tables), 1)
    spread = one_if(
        iota((128, 256 * tables), 0)
        == lax.shift_right_logical(spread_lane, 8) * bucket
        + lax.bitwise_and(spread_lane, bucket - 1)
    )
    lane = iota((peers, 256 * tables), 1)
    own_lane = lax.shift_right_logical(
        lax.bitwise_and(lane, 255), bucket.bit_length() - 1
    ) == lax.bitwise_and(iota((peers, 256 * tables), 0), group - 1)

    def lane_vectors(digit):
        wide = jnp.dot(digit.astype(BF16), spread, preferred_element_type=F32)
        wide = jnp.where(own_lane, wide, F32(0.0)).reshape(chunks, group, 256 * tables)
        return jnp.sum(wide, axis=1)

    lows = lane_vectors(low)
    tiles_of = lane_vectors(tile)
    uppers = lane_vectors(upper)
    upper_t = jnp.concatenate(
        [uppers[:, i * 128 : (i + 1) * 128] for i in range(2 * tables)]
        + [jnp.zeros((128 - 2 * tables * chunks, 128), F32)],
        axis=0,
    ).T
    lane_id = iota((128, 128), 1)
    sub_id = iota((256, 256), 0).astype(F32)

    for t in range(tables):
        for c in range(chunks):
            col = slice(c * 256, (c + 1) * 256)
            low_ref[:, col] = one_if(lows[c : c + 1, t * 256 : (t + 1) * 256] == sub_id)
            hot_ref[:, col] = jnp.broadcast_to(
                tiles_of[c : c + 1, t * 256 : (t + 1) * 256], (16, 256)
            ).astype(BF16)

        def add_chunks(c0, c1, t=t):
            for c in range(c0, c1):
                for h in range(2):
                    k = 2 * t + h
                    is_upper = upper_t[:, k * chunks + c : k * chunks + c + 1]
                    src = slice(c * group + h * group // 2, c * group + (h + 1) * group // 2)
                    terms = got_ref[t, src].reshape(128, width)
                    up = jnp.broadcast_to(is_upper, (128, width)).astype(BF16)
                    row = slice(c * 256 + h * 128, c * 256 + (h + 1) * 128)
                    rhs_ref[row, width:] = terms * up
                    rhs_ref[row, :width] = terms * (BF16(1.0) - up)
            depth = (c1 - c0) * 256
            span = slice(c0 * 256, c1 * 256)

            def tile_step(m, carry):
                hot = hot_ref[:, span]
                low = low_ref[:, span].reshape(16, 16, depth)
                lhs = []
                for i in range(WIDE):
                    at_tile = hot == (WIDE * m + i).astype(F32).astype(BF16)
                    mask = jnp.where(at_tile, BF16(1.0), BF16(0.0))
                    lhs.append((low * mask[None]).reshape(256, depth))
                both = jnp.dot(
                    jnp.concatenate(lhs, axis=0), rhs_ref[span, :], preferred_element_type=F32
                )
                for p in range(2):
                    for h in range(2 * WIDE):
                        s = both[h * 128 : (h + 1) * 128, p * width : (p + 1) * width]
                        block = p * (half // 128) + 2 * WIDE * m + h
                        at = pl.ds(pl.multiple_of(block * 128, 128), 128)
                        if c0 > 0:
                            s = s + sum_ref[t, at, :]
                        sum_ref[t, at, :] = s
                        if c1 == chunks:
                            squares = jnp.sum(s * s, axis=1, keepdims=True)
                            square_ref[...] = jnp.where(
                                lane_id == block * tables + t, squares, square_ref[...]
                            )
                return carry

            lax.fori_loop(0, tiles // WIDE, tile_step, 0, unroll=UNROLL if depth > 1024 else 2)

        if t == 1:
            wait_for(send_ref.at[1], send_sem.at[1], 0, peers - 1)
            send_table(3)
        if t < last:
            wait_for(got_ref.at[t], recv_sem.at[t], 0, peers - 1)
            add_chunks(0, chunks)
        else:
            for (c0, c1), s in zip(tail, tail_sems):
                wait_for(got_ref.at[t], recv_sem.at[s], c0 * group, min(c1 * group, peers - 1))
                add_chunks(c0, c1)
    part_ref[...] = jnp.broadcast_to(
        jnp.sum(square_ref[...], axis=0, keepdims=True), part_ref.shape
    )
    new_acc = acc_t + square_ref[...] * F32(1.0 / width)
    rate = STEP / (jnp.sqrt(new_acc) + EPS)
    nacc_ref[...] = new_acc.T
    for slot in range(peers - 1):
        send(peer_at(slot), part_ref.at[pl.ds(0, 1)], parts_ref.at[slot], parts_sem)
    for t in range(tables):
        loads[t].wait()
        for block in range(rows // 128):
            at = slice(block * 128, (block + 1) * 128)
            lane_at = block * tables + t
            out_ref[t, at, :] = out_ref[t, at, :] - sum_ref[t, at, :] * rate[:, lane_at : lane_at + 1]
    parts_ref[pl.ds(peers - 1, 1)] = part_ref[0:1].reshape(1, 1, 128)
    wait_for(parts_ref, recv_sem.at[parts_sem], 0, peers - 1)
    total = jnp.sum(parts_ref[...].reshape(peers, 128), axis=0, keepdims=True)
    total = jnp.sum(total, axis=1, keepdims=True)
    scale_ref[...] = jnp.broadcast_to(jnp.sqrt(total * F32(1.0 / count)), scale_ref.shape)
    wait_for(send_ref.at[2], send_sem.at[2], 0, peers - 1)
    for (c0, c1), s in zip(tail, tail_sems):
        wait_for(send_ref.at[last], send_sem.at[s], c0 * group, min(c1 * group, peers - 1))
    wait_for(srow_ref, send_sem.at[rows_sem], 0, peers - 1)
    wait_for(parts_ref, send_sem.at[parts_sem], 0, peers - 1)


def write_out(tab_ref, acc_ref, scale_ref, out_ref, nacc_ref, total_ref, sem):
    tables, rows, _ = tab_ref.shape
    stores = [pltpu.make_async_copy(acc_ref, nacc_ref, sem.at[2 * tables])]
    for t in range(tables):
        for h in range(2):
            part = pl.ds(h * rows // 2, rows // 2)
            stores.append(
                pltpu.make_async_copy(
                    tab_ref.at[t, part], out_ref.at[t, part], sem.at[2 * t + h]
                )
            )
    for store in stores:
        store.start()
    total_ref[...] = scale_ref[0:1, 0:1]
    for store in stores:
        store.wait()


def per_device(peers, sizes, lookup_ids, bag_lengths, pooled_gradients, tables, accumulators):
    samples, count_tables, bag_width = lookup_ids.shape
    width = pooled_gradients.shape[2]
    rows_dev = tables.shape[1]
    lookups = samples * bag_width
    bucket = lookups // peers
    blocks = rows_dev // 128
    count = width * count_tables * lookups * peers
    in_vmem = pl.BlockSpec(memory_space=VMEM)
    in_any = pl.BlockSpec(memory_space=pl.ANY)
    in_hbm = pl.BlockSpec(memory_space=pltpu.HBM)
    acc = accumulators.reshape(count_tables, blocks, 128).transpose(1, 0, 2).reshape(-1, 128)
    moved, new_acc, scale = pl.pallas_call(
        functools.partial(
            exchange_and_update, sizes, rows_dev.bit_length() - 1, bucket, count
        ),
        out_shape=(
            VMEM(tables.shape, F32),
            VMEM(acc.shape, F32),
            VMEM((8, 128), F32),
        ),
        in_specs=[in_hbm] * 5,
        out_specs=(in_vmem, in_vmem, in_vmem),
        scratch_shapes=[
            VMEM((count_tables, bag_width, samples), I32),
            VMEM((count_tables, samples), I32),
            VMEM((samples * count_tables, width), BF16),
            VMEM(acc.shape, F32),
            VMEM((count_tables, peers, bucket, width), BF16),
            VMEM((peers, 1, 128), I32),
            VMEM((count_tables, peers, bucket, width), BF16),
            VMEM((peers, 1, 128), I32),
            VMEM((samples * count_tables, width), F32),
            VMEM((count_tables, samples, width), BF16),
            VMEM((peers * bucket, width), F32),
            VMEM(tables.shape, F32),
            VMEM((256, lookups), BF16),
            VMEM((16, lookups), BF16),
            VMEM((lookups, 2 * width), BF16),
            VMEM((128, 128), F32),
            VMEM((8, 128), F32),
            VMEM((peers, 1, 128), F32),
            pltpu.SemaphoreType.DMA((count_tables + 4,)),
            pltpu.SemaphoreType.DMA((count_tables + 3,)),
            pltpu.SemaphoreType.DMA((count_tables + 3,)),
        ],
        compiler_params=pltpu.CompilerParams(
            collective_id=0, has_side_effects=True, vmem_limit_bytes=58_585_088
        ),
        name="exchange",
    )(
        lookup_ids.transpose(1, 2, 0),
        bag_lengths.T,
        pooled_gradients.reshape(samples * count_tables, width),
        acc,
        tables,
    )
    new_tables, new_acc, total = pl.pallas_call(
        write_out,
        out_shape=(
            jax.ShapeDtypeStruct(tables.shape, F32),
            jax.ShapeDtypeStruct(acc.shape, F32),
            jax.ShapeDtypeStruct((1, 1), F32),
        ),
        in_specs=[in_vmem] * 3,
        out_specs=(in_any, in_any, in_vmem),
        scratch_shapes=[pltpu.SemaphoreType.DMA((2 * count_tables + 1,))],
        compiler_params=pltpu.CompilerParams(vmem_limit_bytes=16 * 2**20),
        name="write_out",
    )(moved, new_acc, scale)
    new_acc = new_acc.reshape(blocks, count_tables, 128).transpose(1, 0, 2).reshape(accumulators.shape)
    return (new_tables, new_acc, total[0, 0])


def solution(mesh):
    peers = mesh.devices.size
    return jax.shard_map(
        functools.partial(per_device, peers, (4, 4, 4, 2)),
        mesh=mesh,
        in_specs=(
            P("shard", None, None),
            P("shard", None),
            P("shard", None, None),
            P(None, "shard", None),
            P(None, "shard"),
        ),
        out_specs=(P(None, "shard", None), P(None, "shard"), P()),
        check_vma=False,
    )
```

```python
import functools

import jax
import jax.numpy as jnp
from jax import lax
from jax.experimental import pallas as pl
from jax.experimental.pallas import tpu as pltpu
from jax.sharding import PartitionSpec as P

STEP = 0.5
EPS = 1e-08
F32 = jnp.float32
BF16 = jnp.bfloat16
I32 = jnp.int32
MESH = pl.DeviceIdType.MESH
VMEM = pltpu.VMEM


def iota(shape, dim):
    return lax.broadcasted_iota(I32, shape, dim)


def one_if(mask):
    return jnp.where(mask, F32(1.0), F32(0.0)).astype(BF16)


def nt_dot(a, b):
    return lax.dot_general(a, b, (((1,), (1,)), ((), ())), preferred_element_type=F32)


EVEN = 2
WIDE = 4
UNROLL = 1


def send_order(sizes):
    peers = 1
    for size in sizes:
        peers *= size
    even = []
    for k in range(peers - 1):
        rest = (29 * k) % (peers - 1) + 1
        offset = []
        for size in reversed(sizes):
            offset.insert(0, rest % size)
            rest //= size
        even.append(tuple(offset))

    def hops(offset):
        return sum(min(d, size - d) for d, size in zip(offset[:-1], sizes))

    far = sorted(even, key=lambda offset: -hops(offset))
    return far, [far.index(offset) for offset in even]


def rank_table(t, ids_ref, len_ref, peers, shift, bucket):
    bags = ids_ref.shape[2]
    width = ids_ref.shape[1]
    lens = len_ref[t : t + 1, :]
    owner_iota = iota((peers, bags), 0)
    bag_iota = iota((1, bags), 1).astype(F32)
    upper = one_if(iota((bags, bags), 0) < iota((bags, bags), 1))
    ones = jnp.ones((bags, bags), BF16)
    prefix_rhs = jnp.concatenate([upper, ones], axis=0)
    rank_iota = iota((bucket, bags), 0).astype(F32)
    seen = jnp.zeros((peers, bags), F32)
    owned = []
    values = []
    for l in range(width):
        ids = ids_ref[t, l : l + 1, :]
        owner = lax.shift_right_logical(ids, shift)
        local = lax.bitwise_and(ids, (1 << shift) - 1)
        own32 = jnp.where(owner == owner_iota, F32(1.0), F32(0.0))
        own = own32.astype(BF16)
        before = jnp.dot(
            jnp.concatenate([own, seen.astype(BF16)], axis=1),
            prefix_rhs,
            preferred_element_type=F32,
        )
        rank = jnp.sum(own32 * before, axis=0, keepdims=True)
        seen = seen + own32
        at_rank = rank == rank_iota
        bag = jnp.where(l < lens, bag_iota, F32(bags))
        high = lax.shift_right_logical(local, 6).astype(F32)
        low = lax.bitwise_and(local, 63).astype(F32)
        zero = jnp.zeros_like(rank_iota)
        values.append(
            jnp.concatenate(
                [
                    jnp.where(at_rank, bag, zero),
                    jnp.where(at_rank, high, zero),
                    jnp.where(at_rank, low, zero),
                ],
                axis=0,
            ).astype(BF16)
        )
        owned.append(own)
    table = nt_dot(jnp.concatenate(owned, axis=1), jnp.concatenate(values, axis=1))
    rows = (table[:, bucket : 2 * bucket] * 64.0 + table[:, 2 * bucket :]).astype(I32)
    return table[:, :bucket], rows


def select_table(t, bag_of, scaled_ref, send_ref, rows32_ref):
    peers, bucket = bag_of.shape
    bags = scaled_ref.shape[1]
    lane = iota((peers, bags), 1).astype(F32)
    select = jnp.concatenate([one_if(bag_of[:, r : r + 1] == lane) for r in range(bucket)], axis=0)
    moved = jnp.dot(select, scaled_ref[t], preferred_element_type=F32)
    for r in range(bucket):
        rows32_ref[pl.ds(r, peers, stride=bucket), :] = moved[r * peers : (r + 1) * peers]
    send_ref[t] = rows32_ref[...].reshape(peers, bucket, -1).astype(BF16)


def exchange_and_update(
    sizes,
    shift,
    bucket,
    count,
    ids_hbm,
    len_hbm,
    g_hbm,
    acc_hbm,
    tab_ref,
    out_ref,
    nacc_ref,
    scale_ref,
    ids_ref,
    len_ref,
    g_ref,
    acc_ref,
    send_ref,
    srow_ref,
    got_ref,
    grow_ref,
    g32_ref,
    scaled_ref,
    rows32_ref,
    sum_ref,
    low_ref,
    hot_ref,
    rhs_ref,
    square_ref,
    part_ref,
    parts_ref,
    in_sem,
    send_sem,
    recv_sem,
):
    tables, rows, width = tab_ref.shape
    bags = ids_ref.shape[2]
    peers = send_ref.shape[1]
    lookups = peers * bucket
    group = 256 // bucket
    chunks = peers // group
    half = rows // 2
    tiles = half // 256
    me = lax.axis_index("shard")
    loads = [
        pltpu.make_async_copy(tab_ref.at[t], out_ref.at[t], in_sem.at[t]) for t in range(tables)
    ]
    small = [
        pltpu.make_async_copy(src, dst, in_sem.at[tables + i])
        for i, (src, dst) in enumerate(
            ((ids_hbm, ids_ref), (len_hbm, len_ref), (g_hbm, g_ref), (acc_hbm, acc_ref))
        )
    ]
    for load in small + loads:
        load.start()
    near = []
    span = peers
    for size in sizes:
        span //= size
        here = lax.rem(lax.div(me, span), size)
        near.append([lax.rem(here + d, size) * span for d in range(size)])
    far, even = send_order(sizes)

    def peer_at(slot):
        return sum(spots[d] for spots, d in zip(near, far[slot]))

    barrier = pltpu.get_barrier_semaphore()
    for slot in range(peers - 1):
        pl.semaphore_signal(barrier, inc=1, device_id=(peer_at(slot),), device_id_type=MESH)
    for load in small:
        load.wait()

    g32_ref[...] = g_ref[...].astype(F32)
    lens = len_ref[...].astype(F32)
    lens_t = jnp.concatenate([lens, jnp.ones((128 - tables, bags), F32)], axis=0).T
    for t in range(tables):
        part = g32_ref[pl.ds(t, bags, stride=tables), :]
        scaled_ref[t] = (part / lens_t[:, t : t + 1]).astype(BF16)
    ranked = [rank_table(t, ids_ref, len_ref, peers, shift, bucket) for t in range(tables)]
    srow_ref[...] = jnp.concatenate(
        [r for _, r in ranked] + [jnp.zeros((peers, 128 - tables * bucket), I32)], axis=1
    ).reshape(srow_ref.shape)

    def send(p, src, dst, s):
        pltpu.make_async_remote_copy(
            src_ref=src,
            dst_ref=dst,
            send_sem=send_sem.at[s],
            recv_sem=recv_sem.at[s],
            device_id=(p,),
            device_id_type=MESH,
        ).start()

    last = tables - 1
    rows_sem = tables
    parts_sem = tables + 1
    tail = [(0, chunks // 2), (chunks // 2, chunks)]
    tail_sems = [last, tables + 2]

    def send_table(t):
        for slot in even if t < EVEN else range(peers - 1):
            p = peer_at(slot)
            if t == 0:
                send(p, srow_ref.at[p], grow_ref.at[slot], rows_sem)
            sem = t
            if t == last:
                sem = next(s for (_, c1), s in zip(tail, tail_sems) if slot < c1 * group)
            send(p, send_ref.at[t, p], got_ref.at[t, slot], sem)

    def wait_for(ref, s, begin, end):
        part = ref.at[pl.ds(begin, end - begin)]
        pltpu.make_async_copy(part, part, s).wait()


    select_table(0, ranked[0][0], scaled_ref, send_ref, rows32_ref)
    select_table(1, ranked[1][0], scaled_ref, send_ref, rows32_ref)
    pl.semaphore_wait(barrier, peers - 1)
    send_table(0)
    for t in range(2, tables):
        select_table(t, ranked[t][0], scaled_ref, send_ref, rows32_ref)
        if t == 2:
            send_table(1)
    grow_ref[pl.ds(peers - 1, 1)] = srow_ref[pl.ds(me, 1)]
    for t in range(tables):
        got_ref[t, pl.ds(peers - 1, 1)] = send_ref[t, pl.ds(me, 1)]
    wait_for(send_ref.at[0], send_sem.at[0], 0, peers - 1)
    send_table(2)
    acc_t = acc_ref[...].T
    square_ref[...] = jnp.zeros_like(square_ref)

    wait_for(grow_ref, recv_sem.at[rows_sem], 0, peers - 1)
    got_rows = grow_ref[...].reshape(peers, 128)
    upper = lax.shift_right_logical(got_rows, half.bit_length() - 1)
    tile = lax.shift_right_logical(lax.bitwise_and(got_rows, half - 1), 8)
    low = lax.bitwise_and(got_rows, 255)
    spread_lane = iota((128, 256 * tables), 1)
    spread = one_if(
        iota((128, 256 * tables), 0)
        == lax.shift_right_logical(spread_lane, 8) * bucket
        + lax.bitwise_and(spread_lane, bucket - 1)
    )
    lane = iota((peers, 256 * tables), 1)
    own_lane = lax.shift_right_logical(
        lax.bitwise_and(lane, 255), bucket.bit_length() - 1
    ) == lax.bitwise_and(iota((peers, 256 * tables), 0), group - 1)

    def lane_vectors(digit):
        wide = jnp.dot(digit.astype(BF16), spread, preferred_element_type=F32)
        wide = jnp.where(own_lane, wide, F32(0.0)).reshape(chunks, group, 256 * tables)
        return jnp.sum(wide, axis=1)

    lows = lane_vectors(low)
    tiles_of = lane_vectors(tile)
    uppers = lane_vectors(upper)
    upper_t = jnp.concatenate(
        [uppers[:, i * 128 : (i + 1) * 128] for i in range(2 * tables)]
        + [jnp.zeros((128 - 2 * tables * chunks, 128), F32)],
        axis=0,
    ).T
    lane_id = iota((128, 128), 1)
    sub_id = iota((256, 256), 0).astype(F32)

    for t in range(tables):
        for c in range(chunks):
            col = slice(c * 256, (c + 1) * 256)
            low_ref[:, col] = one_if(lows[c : c + 1, t * 256 : (t + 1) * 256] == sub_id)
            hot_ref[:, col] = jnp.broadcast_to(
                tiles_of[c : c + 1, t * 256 : (t + 1) * 256], (16, 256)
            ).astype(BF16)

        def add_chunks(c0, c1, t=t):
            for c in range(c0, c1):
                for h in range(2):
                    k = 2 * t + h
                    is_upper = upper_t[:, k * chunks + c : k * chunks + c + 1]
                    src = slice(c * group + h * group // 2, c * group + (h + 1) * group // 2)
                    terms = got_ref[t, src].reshape(128, width)
                    up = jnp.broadcast_to(is_upper, (128, width)).astype(BF16)
                    row = slice(c * 256 + h * 128, c * 256 + (h + 1) * 128)
                    rhs_ref[row, width:] = terms * up
                    rhs_ref[row, :width] = terms * (BF16(1.0) - up)
            depth = (c1 - c0) * 256
            span = slice(c0 * 256, c1 * 256)

            def tile_step(m, carry):
                hot = hot_ref[:, span]
                low = low_ref[:, span].reshape(16, 16, depth)
                lhs = []
                for i in range(WIDE):
                    at_tile = hot == (WIDE * m + i).astype(F32).astype(BF16)
                    mask = jnp.where(at_tile, BF16(1.0), BF16(0.0))
                    lhs.append((low * mask[None]).reshape(256, depth))
                both = jnp.dot(
                    jnp.concatenate(lhs, axis=0), rhs_ref[span, :], preferred_element_type=F32
                )
                for p in range(2):
                    for h in range(2 * WIDE):
                        s = both[h * 128 : (h + 1) * 128, p * width : (p + 1) * width]
                        block = p * (half // 128) + 2 * WIDE * m + h
                        at = pl.ds(pl.multiple_of(block * 128, 128), 128)
                        if c0 > 0:
                            s = s + sum_ref[t, at, :]
                        sum_ref[t, at, :] = s
                        if c1 == chunks:
                            squares = jnp.sum(s * s, axis=1, keepdims=True)
                            square_ref[...] = jnp.where(
                                lane_id == block * tables + t, squares, square_ref[...]
                            )
                return carry

            lax.fori_loop(0, tiles // WIDE, tile_step, 0, unroll=UNROLL if depth > 1024 else 2)

        if t == 1:
            wait_for(send_ref.at[1], send_sem.at[1], 0, peers - 1)
            send_table(3)
        if t < last:
            wait_for(got_ref.at[t], recv_sem.at[t], 0, peers - 1)
            add_chunks(0, chunks)
        else:
            for (c0, c1), s in zip(tail, tail_sems):
                wait_for(got_ref.at[t], recv_sem.at[s], c0 * group, min(c1 * group, peers - 1))
                add_chunks(c0, c1)
    part_ref[...] = jnp.broadcast_to(
        jnp.sum(square_ref[...], axis=0, keepdims=True), part_ref.shape
    )
    new_acc = acc_t + square_ref[...] * F32(1.0 / width)
    rate = STEP / (jnp.sqrt(new_acc) + EPS)
    for slot in range(peers - 1):
        send(peer_at(slot), part_ref.at[pl.ds(0, 1)], parts_ref.at[slot], parts_sem)
    nacc_ref[...] = new_acc.T
    for t in range(tables):
        loads[t].wait()
        for block in range(rows // 128):
            at = slice(block * 128, (block + 1) * 128)
            lane_at = block * tables + t
            out_ref[t, at, :] = out_ref[t, at, :] - sum_ref[t, at, :] * rate[:, lane_at : lane_at + 1]
    parts_ref[pl.ds(peers - 1, 1)] = part_ref[0:1].reshape(1, 1, 128)
    wait_for(parts_ref, recv_sem.at[parts_sem], 0, peers - 1)
    total = jnp.sum(parts_ref[...].reshape(peers, 128), axis=0, keepdims=True)
    total = jnp.sum(total, axis=1, keepdims=True)
    scale_ref[...] = jnp.broadcast_to(jnp.sqrt(total * F32(1.0 / count)), scale_ref.shape)
    wait_for(send_ref.at[2], send_sem.at[2], 0, peers - 1)
    for (c0, c1), s in zip(tail, tail_sems):
        wait_for(send_ref.at[last], send_sem.at[s], c0 * group, min(c1 * group, peers - 1))
    wait_for(srow_ref, send_sem.at[rows_sem], 0, peers - 1)
    wait_for(parts_ref, send_sem.at[parts_sem], 0, peers - 1)


def write_out(tab_ref, acc_ref, scale_ref, out_ref, nacc_ref, total_ref, sem):
    tables, rows, _ = tab_ref.shape
    stores = [pltpu.make_async_copy(acc_ref, nacc_ref, sem.at[2 * tables])]
    for t in range(tables):
        for h in range(2):
            part = pl.ds(h * rows // 2, rows // 2)
            stores.append(
                pltpu.make_async_copy(
                    tab_ref.at[t, part], out_ref.at[t, part], sem.at[2 * t + h]
                )
            )
    for store in stores:
        store.start()
    total_ref[...] = scale_ref[0:1, 0:1]
    for store in stores:
        store.wait()


def per_device(peers, sizes, lookup_ids, bag_lengths, pooled_gradients, tables, accumulators):
    samples, count_tables, bag_width = lookup_ids.shape
    width = pooled_gradients.shape[2]
    rows_dev = tables.shape[1]
    lookups = samples * bag_width
    bucket = lookups // peers
    blocks = rows_dev // 128
    count = width * count_tables * lookups * peers
    in_vmem = pl.BlockSpec(memory_space=VMEM)
    in_any = pl.BlockSpec(memory_space=pl.ANY)
    in_hbm = pl.BlockSpec(memory_space=pltpu.HBM)
    acc = accumulators.reshape(count_tables, blocks, 128).transpose(1, 0, 2).reshape(-1, 128)
    moved, new_acc, scale = pl.pallas_call(
        functools.partial(
            exchange_and_update, sizes, rows_dev.bit_length() - 1, bucket, count
        ),
        out_shape=(
            VMEM(tables.shape, F32),
            VMEM(acc.shape, F32),
            VMEM((8, 128), F32),
        ),
        in_specs=[in_hbm] * 5,
        out_specs=(in_vmem, in_vmem, in_vmem),
        scratch_shapes=[
            VMEM((count_tables, bag_width, samples), I32),
            VMEM((count_tables, samples), I32),
            VMEM((samples * count_tables, width), BF16),
            VMEM(acc.shape, F32),
            VMEM((count_tables, peers, bucket, width), BF16),
            VMEM((peers, 1, 128), I32),
            VMEM((count_tables, peers, bucket, width), BF16),
            VMEM((peers, 1, 128), I32),
            VMEM((samples * count_tables, width), F32),
            VMEM((count_tables, samples, width), BF16),
            VMEM((peers * bucket, width), F32),
            VMEM(tables.shape, F32),
            VMEM((256, lookups), BF16),
            VMEM((16, lookups), BF16),
            VMEM((lookups, 2 * width), BF16),
            VMEM((128, 128), F32),
            VMEM((8, 128), F32),
            VMEM((peers, 1, 128), F32),
            pltpu.SemaphoreType.DMA((count_tables + 4,)),
            pltpu.SemaphoreType.DMA((count_tables + 3,)),
            pltpu.SemaphoreType.DMA((count_tables + 3,)),
        ],
        compiler_params=pltpu.CompilerParams(
            collective_id=0, has_side_effects=True, vmem_limit_bytes=58_585_088
        ),
        name="exchange",
    )(
        lookup_ids.transpose(1, 2, 0),
        bag_lengths.T,
        pooled_gradients.reshape(samples * count_tables, width),
        acc,
        tables,
    )
    new_tables, new_acc, total = pl.pallas_call(
        write_out,
        out_shape=(
            jax.ShapeDtypeStruct(tables.shape, F32),
            jax.ShapeDtypeStruct(acc.shape, F32),
            jax.ShapeDtypeStruct((1, 1), F32),
        ),
        in_specs=[in_vmem] * 3,
        out_specs=(in_any, in_any, in_vmem),
        scratch_shapes=[pltpu.SemaphoreType.DMA((2 * count_tables + 1,))],
        compiler_params=pltpu.CompilerParams(vmem_limit_bytes=16 * 2**20),
        name="write_out",
    )(moved, new_acc, scale)
    new_acc = new_acc.reshape(blocks, count_tables, 128).transpose(1, 0, 2).reshape(accumulators.shape)
    return (new_tables, new_acc, total[0, 0])


def solution(mesh):
    peers = mesh.devices.size
    return jax.shard_map(
        functools.partial(per_device, peers, (4, 4, 4, 2)),
        mesh=mesh,
        in_specs=(
            P("shard", None, None),
            P("shard", None),
            P("shard", None, None),
            P(None, "shard", None),
            P(None, "shard"),
        ),
        out_specs=(P(None, "shard", None), P(None, "shard"), P()),
        check_vma=False,
    )
```
